64 devices in a mesh: rep: 4 (over x, y), dp: 16 (over z, core).
Axes of the slice: x: 2, y: 2, z: 8, core: 2. Of those that a mesh axis runs over, the one named last changes fastest.
The devices are a block of a 4x4x8 slice.
Arguments:
- g_w_gate: bfloat16 [64, 2, 896, 2560], P(('rep', 'dp')), parts along dimension 0
- g_w_up: bfloat16 [64, 2, 896, 2560], P(('rep', 'dp')), parts along dimension 0
- g_w_down: bfloat16 [64, 2, 2560, 896], P(('rep', 'dp')), parts along dimension 0
- w_gate: bfloat16 [2, 896, 2560], replicated
- w_up: bfloat16 [2, 896, 2560], replicated
- w_down: bfloat16 [2, 2560, 896], replicated
- m_w_gate: float32 [2, 896, 2560], P(None, 'dp')
- m_w_up: float32 [2, 896, 2560], P(None, 'dp')
- m_w_down: float32 [2, 2560, 896], P(None, 'dp')
- v_w_gate: float32 [2, 896, 2560], P(None, 'dp')
- v_w_up: float32 [2, 896, 2560], P(None, 'dp')
- v_w_down: float32 [2, 2560, 896], P(None, 'dp')
Outputs:
- output 1: bfloat16 [8, 896, 2560], P('rep'), parts along dimension 0
- output 2: bfloat16 [8, 896, 2560], P('rep'), parts along dimension 0
- output 3: bfloat16 [8, 2560, 896], P('rep'), parts along dimension 0
- output 4: float32 [8, 896, 2560], P('rep', 'dp'), parts along dimension 0
- output 5: float32 [8, 896, 2560], P('rep', 'dp'), parts along dimension 0
- output 6: float32 [8, 2560, 896], P('rep', 'dp'), parts along dimension 0
- output 7: float32 [8, 896, 2560], P('rep', 'dp'), parts along dimension 0
- output 8: float32 [8, 896, 2560], P('rep', 'dp'), parts along dimension 0
- output 9: float32 [8, 2560, 896], P('rep', 'dp'), parts along dimension 0
There are 4 independent parts. The reference program is written for one: setup_inputs(seed, part) draws one part's arguments, and reference() takes and returns one part's arrays. A program takes and returns all parts, laid end to end along the dimension named above; an argument that names none is the same for every part.
All inputs are finite; a program needn't handle non-finite values.
Results may differ from the reference program's by a relative error of at most 0.022.
Values are sent between devices in bfloat16 or wider.
A program may use at most 768 MiB of HBM per device.

```python
import jax
import jax.numpy as jnp
from jax import lax

DEVICES = 16
D = 896
FF = 2560
LAYERS = 2
NAMES = ("w_gate", "w_up", "w_down")
SHAPES = {"w_gate": (LAYERS, D, FF), "w_up": (LAYERS, D, FF), "w_down": (LAYERS, FF, D)}


def setup_inputs(seed: int = 0, part: int = 0) -> dict:
    kz, *keys = jax.random.split(jax.random.key(seed), 1 + 5 * len(NAMES))
    loud = 2.0 ** jax.random.uniform(kz, (), jnp.float32, -1.0, 1.0)
    drawn = {}
    for name, key, both in zip(NAMES, keys[:3], keys[3:6], strict=True):
        own = jax.random.normal(jax.random.fold_in(key, part), (DEVICES, *SHAPES[name]), jnp.float32)
        shared = jax.random.normal(jax.random.fold_in(both, part), SHAPES[name], jnp.float32)
        drawn["g_" + name] = (loud * (0.7 * shared / DEVICES + 0.7 * own * DEVICES**-0.5)).astype(jnp.bfloat16)
    for name, key in zip(NAMES, keys[6:9], strict=True):
        drawn[name] = (jax.random.normal(key, SHAPES[name], jnp.float32) * SHAPES[name][1] ** -0.5).astype(jnp.bfloat16)
    for name, key in zip(NAMES, keys[9:12], strict=True):
        drawn["m_" + name] = loud * 0.5 * jax.random.normal(key, SHAPES[name], jnp.float32)
    for name, key in zip(NAMES, keys[12:15], strict=True):
        drawn["v_" + name] = loud * loud * jax.random.uniform(key, SHAPES[name], jnp.float32, 0.5, 1.5)
    return drawn


def adamw(w, m, v, g):
    m = 0.9 * m + 0.1 * g
    v = 0.95 * v + 0.05 * g * g
    step = m * lax.rsqrt(v + 1e-8) + 0.1 * w
    return (w - 0.02 * step).astype(jnp.bfloat16), m, v


def reference(g_w_gate, g_w_up, g_w_down, w_gate, w_up, w_down, m_w_gate, m_w_up, m_w_down, v_w_gate, v_w_up, v_w_down):
    def total(terms):
        return lax.scan(lambda so_far, term: (so_far + term.astype(jnp.float32), None), jnp.zeros(terms.shape[1:], jnp.float32), terms)[0]

    gradients = [total(terms).astype(jnp.bfloat16).astype(jnp.float32) for terms in (g_w_gate, g_w_up, g_w_down)]
    new = [
        adamw(w.astype(jnp.float32), m, v, g)
        for w, m, v, g in zip((w_gate, w_up, w_down), (m_w_gate, m_w_up, m_w_down), (v_w_gate, v_w_up, v_w_down), gradients, strict=True)
    ]
    return tuple(one[which] for which in range(3) for one in new)
```

```python
import functools

import jax
import jax.numpy as jnp
from jax import lax
from jax.experimental import pallas as pl
from jax.experimental.pallas import tpu as pltpu
from jax.sharding import PartitionSpec as P

CORES = 2
SUBLANES = 8
VMEM_LIMIT = 20 * 2**20


def adamw(w, m, v, g):
    m = 0.9 * m + 0.1 * g
    v = 0.95 * v + 0.05 * g * g
    step = m * lax.rsqrt(v + 1e-8) + 0.1 * w
    return (w - 0.02 * step).astype(jnp.bfloat16), m, v


def kernel(n, units, *refs):
    g, w, m_in, v_in, out, m, v = (refs[i * units : (i + 1) * units] for i in range(7))
    own, part, w_own = (refs[i * units : (i + 1) * units] for i in (7, 8, 9))
    g = refs[:units]
    scratch = refs[10 * units :]
    own_sem, state_sem, push_send, push_recv, sum_send, sum_recv, new_send, new_recv, pass_send, pass_recv = scratch

    me = lax.axis_index("dp")
    z, core = me // CORES, me % CORES
    ring = n // CORES
    partner = z * CORES + 1 - core
    last = ring - 1
    ways = (1, -1)

    def chip(offset):
        return lax.rem(z + offset + 2 * ring, ring)

    def owner(d, k):
        return chip(-ways[d] * (k + 1))

    def to(index):
        return {"device_id": {"dp": index}, "device_id_type": pl.DeviceIdType.MESH}

    def following(d):
        return to(chip(ways[d]) * CORES + core)

    def load_own(d, k, u):
        slot = lax.rem(k, 2)
        return pltpu.make_async_copy(g[u].at[d, owner(d, k) * CORES + core], own[u].at[slot, d], own_sem.at[slot, d, u])

    def push(d, k, u):
        return pltpu.make_async_remote_copy(
            g[u].at[d, owner(d, k) * CORES + 1 - core], part[u].at[d, k], push_send.at[d, k, u], push_recv.at[d, k, u], **to(partner)
        )

    def send_sum(d, k, u):
        block = out[u].at[d, owner(d, k) * CORES + core]
        return pltpu.make_async_remote_copy(block, block, sum_send.at[d, k, u], sum_recv.at[d, k, u], **following(d))

    def send_new(d, j, u):
        block = out[u].at[d, chip(-ways[d] * j) * CORES + core]
        return pltpu.make_async_remote_copy(block, block, new_send.at[d, j, u], new_recv.at[d, j, u], **following(d))

    def pass_new(d, j, u):
        block = out[u].at[d, chip(-ways[d] * j) * CORES + core]
        return pltpu.make_async_remote_copy(block, block, pass_send.at[d, j, u], pass_recv.at[d, j, u], **to(partner))

    def load_state(d, u):
        return (
            pltpu.make_async_copy(w[u].at[d, me], w_own[u].at[d], state_sem.at[0, d, u]),
            pltpu.make_async_copy(m_in[u].at[d], m[u].at[d], state_sem.at[1, d, u]),
            pltpu.make_async_copy(v_in[u].at[d], v[u].at[d], state_sem.at[2, d, u]),
        )

    every = [(u, d) for u in range(units) for d in range(2)]

    for u, d in every:
        load_own(d, 0, u).start()

    barrier = pltpu.get_barrier_semaphore()
    for index in (chip(1) * CORES + core, chip(-1) * CORES + core, partner):
        pl.semaphore_signal(barrier, inc=1, **to(index))
    pl.semaphore_wait(barrier, 3)

    for k in (0, 1):
        for u, d in every:
            push(d, k, u).start()

    def add(d, k, u, arrived):
        slot, block = lax.rem(k, 2), owner(d, k) * CORES + core
        load_own(d, k, u).wait()
        push(d, k, u).wait_recv()

        @pl.loop(0, own[u].shape[2])
        def _(row):
            total = own[u][slot, d, row].astype(jnp.float32) + part[u][d, k, row].astype(jnp.float32)
            if arrived:
                total = out[u][d, block, row].astype(jnp.float32) + total
            out[u][d, block, row] = total.astype(out[u].dtype)

    for u, d in every:
        load_own(d, 1, u).start()
    for u, d in every:
        add(d, 0, u, False)
        send_sum(d, 0, u).start()
    for u, d in every:
        for copy in load_state(d, u):
            copy.start()

    @pl.loop(1, last)
    def _(k):
        for u, d in every:
            load_own(d, k + 1, u).start()
            push(d, k + 1, u).start()
        for u, d in every:
            send_sum(d, k - 1, u).wait_recv()
            add(d, k, u, True)
            send_sum(d, k - 1, u).wait_send()
            send_sum(d, k, u).start()

    for u, d in every:
        slot = last % 2
        load_own(d, last, u).wait()
        push(d, last, u).wait_recv()
        for copy in load_state(d, u):
            copy.wait()
        send_sum(d, last - 1, u).wait_recv()

        @pl.loop(0, own[u].shape[2])
        def _(row):
            total = own[u][slot, d, row].astype(jnp.float32) + part[u][d, last, row].astype(jnp.float32)
            total = out[u][d, me, row].astype(jnp.float32) + total
            gradient = total.astype(jnp.bfloat16).astype(jnp.float32)
            new = adamw(w_own[u][d, row].astype(jnp.float32), m[u][d, row], v[u][d, row], gradient)
            out[u][d, me, row], m[u][d, row], v[u][d, row] = new

        send_sum(d, last - 1, u).wait_send()
        send_new(d, 0, u).start()
        pass_new(d, 0, u).start()

    @pl.loop(1, last)
    def _(j):
        for u, d in every:
            send_new(d, j - 1, u).wait_recv()
            send_new(d, j, u).start()
            pass_new(d, j, u).start()

    for u, d in every:
        send_new(d, last - 1, u).wait_recv()
        pass_new(d, last, u).start()

    @pl.loop(0, ring)
    def _(j):
        for u, d in every:
            push(d, j, u).wait_send()
            pass_new(d, j, u).wait()

    @pl.loop(0, last)
    def _(j):
        for u, d in every:
            send_new(d, j, u).wait_send()


def place(*refs):
    count = (len(refs) - 1) // 2
    copies = [pltpu.make_async_copy(refs[i], refs[count + i], refs[-1].at[i]) for i in range(count)]
    for copy in copies:
        copy.start()
    for copy in copies:
        copy.wait()


def solution(mesh):
    n = mesh.shape["dp"]

    def step(*arrays):
        terms, weights, m, v = (arrays[i : i + 3] for i in (0, 3, 6, 9))
        units = len(terms)
        layers = weights[0].shape[0]

        def blocks(x, count):
            return x.reshape(layers, *([count] if count else []), -1, SUBLANES, x.shape[-1])

        terms = [blocks(t[0], n) for t in terms]
        weights_in = [blocks(x, n) for x in weights]
        m_in = [blocks(x, 0) for x in m]
        v_in = [blocks(x, 0) for x in v]
        ring = n // CORES
        block = [x.shape[1:] for x in m_in]
        dma = lambda *shape: pltpu.SemaphoreType.DMA(shape)
        new = pl.pallas_call(
            functools.partial(kernel, n, units),
            out_shape=[pltpu.VMEM(x.shape, x.dtype) for x in (*weights_in, *m_in, *v_in)],
            in_specs=[pl.BlockSpec(memory_space=pltpu.HBM)] * (4 * units),
            out_specs=[pl.BlockSpec(memory_space=pltpu.VMEM)] * (3 * units),
            scratch_shapes=[
                *(pltpu.VMEM((2, 2, *b), jnp.bfloat16) for b in block),
                *(pltpu.VMEM((2, ring, *b), jnp.bfloat16) for b in block),
                *(pltpu.VMEM((2, *b), jnp.bfloat16) for b in block),
                dma(2, 2, units),
                dma(3, 2, units),
                *[dma(2, ring, units) for _ in range(8)],
            ],
            compiler_params=pltpu.CompilerParams(collective_id=0, has_side_effects=True, vmem_limit_bytes=VMEM_LIMIT),
            name="step_end",
        )(*(pltpu.with_memory_space_constraint(x, pltpu.HBM) for x in (*terms, *weights_in, *m_in, *v_in)))
        new = pl.pallas_call(
            place,
            out_shape=[jax.ShapeDtypeStruct(x.shape, x.dtype) for x in new],
            in_specs=[pl.BlockSpec(memory_space=pltpu.VMEM)] * len(new),
            out_specs=[pl.BlockSpec(memory_space=pltpu.HBM)] * len(new),
            scratch_shapes=[dma(len(new))],
            compiler_params=pltpu.CompilerParams(vmem_limit_bytes=VMEM_LIMIT),
            name="place",
        )(*(pltpu.with_memory_space_constraint(x, pltpu.VMEM) for x in new))
        return tuple(x.reshape(like.shape) for x, like in zip(new, (*weights, *m, *v), strict=True))

    all_of, cut = P(None, None, None), P(None, "dp", None)
    return jax.shard_map(
        step,
        mesh=mesh,
        in_specs=(P(("rep", "dp"), None, None, None),) * 3 + (all_of,) * 3 + (cut,) * 6,
        out_specs=(P("rep", None, None),) * 3 + (P("rep", "dp", None),) * 6,
        check_vma=False,
    )
```

```python
import functools

import jax
import jax.numpy as jnp
from jax import lax
from jax.experimental import pallas as pl
from jax.experimental.pallas import tpu as pltpu
from jax.sharding import PartitionSpec as P

CORES = 2
SUBLANES = 8
VMEM_LIMIT = 20 * 2**20


def adamw(w, m, v, g):
    m = 0.9 * m + 0.1 * g
    v = 0.95 * v + 0.05 * g * g
    step = m * lax.rsqrt(v + 1e-8) + 0.1 * w
    return (w - 0.02 * step).astype(jnp.bfloat16), m, v


def cuts(rows):
    a = max(rows // 8, 1)
    b = max(rows // 3, a + 1)
    return (0, a), (a, b - a), (b, rows - b)


def kernel(n, units, *refs):
    g, w, m_in, v_in, out, m, v, own, part, w_own = (refs[i * units : (i + 1) * units] for i in range(10))
    own_sem, state_sem, push_send, push_recv, ring_send, ring_recv, pass_send, pass_recv, first_recv, tail_recv = refs[10 * units :]

    me = lax.axis_index("dp")
    z, core = me // CORES, me % CORES
    ring = n // CORES
    partner = z * CORES + 1 - core
    last = ring - 1
    ways = (0, 1)
    final = units - 1

    def chip(offset):
        return lax.rem(z + offset + 2 * ring, ring)

    def behind(d, j):
        return chip(j if d else -j)

    def owner(d, k):
        return behind(d, k + 1)

    def to(index):
        return {"device_id": {"dp": index}, "device_id_type": pl.DeviceIdType.MESH}

    def following(d):
        return to(behind(d, -1) * CORES + core)

    def wait_bytes(ref, sem):
        pltpu.make_async_copy(ref, ref, sem).wait()

    def load_own(k, u):
        slot = lax.rem(k, 2)
        for d in ways:
            pltpu.make_async_copy(g[u].at[d, owner(d, k) * CORES + core], own[u].at[slot, d], own_sem.at[slot, u]).start()

    def push(d, k, u, sem, rows=slice(None)):
        pltpu.make_async_remote_copy(
            g[u].at[d, owner(d, k) * CORES + 1 - core, rows], part[u].at[d, k, rows], push_send.at[d, u], sem, **to(partner)
        ).start()

    def push_all(k, u):
        for d in ways:
            push(d, k, u, push_recv.at[k, u])

    def terms_here(k, u):
        wait_bytes(own[u].at[lax.rem(k, 2)], own_sem.at[lax.rem(k, 2), u])
        wait_bytes(part[u].at[:, k], push_recv.at[k, u])

    def send(block, d, t, u, rows=slice(None), sem=None):
        piece = out[u].at[d, block, rows]
        sem = ring_recv.at[lax.rem(t, 3), d, u] if sem is None else sem
        pltpu.make_async_remote_copy(piece, piece, ring_send.at[d, u], sem, **following(d)).start()

    def sent(d, u):
        wait_bytes(out[u].at[d, 0], ring_send.at[d, u])

    def arrived(block, d, t, u):
        wait_bytes(out[u].at[d, block], ring_recv.at[lax.rem(t, 3), d, u])

    def pass_on(block, d, u, rows=slice(None)):
        piece = out[u].at[d, block, rows]
        pltpu.make_async_remote_copy(piece, piece, pass_send.at[d, u], pass_recv.at[d, u], **to(partner)).start()

    def terms(slot, d, k, u, row):
        return own[u][slot, d, row].astype(jnp.float32) + part[u][d, k, row].astype(jnp.float32)

    rows_of = [x.shape[2] for x in own]

    for u in range(units):
        load_own(0, u)

    barrier = pltpu.get_barrier_semaphore()
    for index in (chip(1) * CORES + core, chip(-1) * CORES + core, partner):
        pl.semaphore_signal(barrier, inc=1, **to(index))
    pl.semaphore_wait(barrier, 3)

    for p, (at, count) in enumerate(cuts(rows_of[0])):
        for d in ways:
            push(d, 0, 0, first_recv.at[d, p], pl.ds(at, count))
    for u in range(1, units):
        push_all(0, u)
    for u in range(units):
        load_own(1, u)
        push_all(1, u)

    def begin(d, u, at, count):
        block = owner(d, 0) * CORES + core

        @pl.loop(at, at + count)
        def _(row):
            out[u][d, block, row] = terms(0, d, 0, u, row).astype(out[u].dtype)

        send(block, d, 0, u, pl.ds(at, count))

    wait_bytes(own[0].at[0], own_sem.at[0, 0])
    for p, (at, count) in enumerate(cuts(rows_of[0])):
        for d in ways:
            wait_bytes(part[0].at[d, 0, pl.ds(at, count)], first_recv.at[d, p])
            begin(d, 0, at, count)
    for u in range(1, units):
        terms_here(0, u)
        for d in ways:
            begin(d, u, 0, rows_of[u])

    state = []
    for u in range(units):
        state.append(
            (
                pltpu.make_async_copy(w[u].at[:, me], w_own[u], state_sem.at[0, u]),
                pltpu.make_async_copy(m_in[u], m[u], state_sem.at[1, u]),
                pltpu.make_async_copy(v_in[u], v[u], state_sem.at[2, u]),
            )
        )
        for copy in state[u]:
            copy.start()

    @pl.loop(1, last)
    def _(k):
        slot = lax.rem(k, 2)
        for u in range(units):
            load_own(k + 1, u)
            push_all(k + 1, u)
        for u in range(units):
            terms_here(k, u)
            for d in ways:
                block = owner(d, k) * CORES + core
                arrived(block, d, k - 1, u)

                @pl.loop(0, rows_of[u])
                def _(row):
                    total = out[u][d, block, row].astype(jnp.float32) + terms(slot, d, k, u, row)
                    out[u][d, block, row] = total.astype(out[u].dtype)

                sent(d, u)
                send(block, d, k, u)

    for u in range(units):
        terms_here(last, u)
        for copy in state[u]:
            copy.wait()
        for d in ways:
            arrived(me, d, last - 1, u)

            @pl.loop(0, rows_of[u])
            def _(row):
                total = out[u][d, me, row].astype(jnp.float32) + terms(last % 2, d, last, u, row)
                gradient = total.astype(jnp.bfloat16).astype(jnp.float32)
                new = adamw(w_own[u][d, row].astype(jnp.float32), m[u][d, row], v[u][d, row], gradient)
                out[u][d, me, row], m[u][d, row], v[u][d, row] = new

            sent(d, u)
            send(me, d, last, u)
            pass_on(me, d, u)

    @pl.loop(1, last - 1)
    def _(j):
        for u in range(units):
            for d in ways:
                block = behind(d, j) * CORES + core
                arrived(block, d, last + j - 1, u)
                sent(d, u)
                send(block, d, last + j, u)
                pass_on(block, d, u)

    for u in range(units):
        for d in ways:
            block = behind(d, last - 1) * CORES + core
            arrived(block, d, 2 * last - 2, u)
            sent(d, u)
            if u == final:
                for p, (at, count) in enumerate(cuts(rows_of[u])[::-1]):
                    send(block, d, 2 * last - 1, u, pl.ds(at, count), tail_recv.at[d, p])
            else:
                send(block, d, 2 * last - 1, u)
            pass_on(block, d, u)

    for u in range(final):
        for d in ways:
            block = behind(d, last) * CORES + core
            arrived(block, d, 2 * last - 1, u)
            pass_on(block, d, u)
    for p, (at, count) in enumerate(cuts(rows_of[final])[::-1]):
        for d in ways:
            block = behind(d, last) * CORES + core
            wait_bytes(out[final].at[d, block, pl.ds(at, count)], tail_recv.at[d, p])
            pass_on(block, d, final, pl.ds(at, count))

    for u in range(units):
        for d in ways:
            sent(d, u)
            wait_bytes(part[u].at[d], push_send.at[d, u])
            wait_bytes(out[u].at[d, pl.ds(0, ring)], pass_send.at[d, u])
            wait_bytes(out[u].at[d, pl.ds(0, ring)], pass_recv.at[d, u])


def place(*refs):
    count = (len(refs) - 1) // 2
    copies = [pltpu.make_async_copy(refs[i], refs[count + i], refs[-1].at[i]) for i in range(count)]
    for copy in copies:
        copy.start()
    for copy in copies:
        copy.wait()


def solution(mesh):
    n = mesh.shape["dp"]

    def step(*arrays):
        terms, weights, m, v = (arrays[i : i + 3] for i in (0, 3, 6, 9))
        units = len(terms)
        layers = weights[0].shape[0]

        def blocks(x, count):
            return x.reshape(layers, *([count] if count else []), -1, SUBLANES, x.shape[-1])

        terms = [blocks(t[0], n) for t in terms]
        weights_in = [blocks(x, n) for x in weights]
        m_in = [blocks(x, 0) for x in m]
        v_in = [blocks(x, 0) for x in v]
        ring = n // CORES
        block = [x.shape[1:] for x in m_in]
        dma = lambda *shape: pltpu.SemaphoreType.DMA(shape)
        new = pl.pallas_call(
            functools.partial(kernel, n, units),
            out_shape=[pltpu.VMEM(x.shape, x.dtype) for x in (*weights_in, *m_in, *v_in)],
            in_specs=[pl.BlockSpec(memory_space=pltpu.HBM)] * (4 * units),
            out_specs=[pl.BlockSpec(memory_space=pltpu.VMEM)] * (3 * units),
            scratch_shapes=[
                *(pltpu.VMEM((2, 2, *b), jnp.bfloat16) for b in block),
                *(pltpu.VMEM((2, ring, *b), jnp.bfloat16) for b in block),
                *(pltpu.VMEM((2, *b), jnp.bfloat16) for b in block),
                dma(2, units),
                dma(3, units),
                dma(2, units),
                dma(ring, units),
                dma(2, units),
                dma(3, 2, units),
                dma(2, units),
                dma(2, units),
                dma(2, 3),
                dma(2, 3),
            ],
            compiler_params=pltpu.CompilerParams(collective_id=0, has_side_effects=True, vmem_limit_bytes=VMEM_LIMIT),
            name="step_end",
        )(*(pltpu.with_memory_space_constraint(x, pltpu.HBM) for x in (*terms, *weights_in, *m_in, *v_in)))
        new = pl.pallas_call(
            place,
            out_shape=[jax.ShapeDtypeStruct(x.shape, x.dtype) for x in new],
            in_specs=[pl.BlockSpec(memory_space=pltpu.VMEM)] * len(new),
            out_specs=[pl.BlockSpec(memory_space=pltpu.HBM)] * len(new),
            scratch_shapes=[dma(len(new))],
            compiler_params=pltpu.CompilerParams(vmem_limit_bytes=VMEM_LIMIT),
            name="place",
        )(*(pltpu.with_memory_space_constraint(x, pltpu.VMEM) for x in new))
        return tuple(x.reshape(like.shape) for x, like in zip(new, (*weights, *m, *v), strict=True))

    all_of, cut = P(None, None, None), P(None, "dp", None)
    return jax.shard_map(
        step,
        mesh=mesh,
        in_specs=(P(("rep", "dp"), None, None, None),) * 3 + (all_of,) * 3 + (cut,) * 6,
        out_specs=(P("rep", None, None),) * 3 + (P("rep", "dp", None),) * 6,
        check_vma=False,
    )
```

```python
import functools

import jax
import jax.numpy as jnp
from jax import lax
from jax.experimental import pallas as pl
from jax.experimental.pallas import tpu as pltpu
from jax.sharding import PartitionSpec as P

CORES = 2
SUBLANES = 8
VMEM_LIMIT = 20 * 2**20


def adamw(w, m, v, g):
    m = 0.9 * m + 0.1 * g
    v = 0.95 * v + 0.05 * g * g
    step = m * lax.rsqrt(v + 1e-8) + 0.1 * w
    return (w - 0.02 * step).astype(jnp.bfloat16), m, v


def cuts(rows):
    a = max(rows // 8, 1)
    b = max(rows // 3, a + 1)
    return (0, a), (a, b - a), (b, rows - b)


def kernel(n, order, late, *refs):
    units = len(order)
    g, w, m_in, v_in, out, m, v = (refs[i * units : (i + 1) * units] for i in range(7))
    after, refs = refs[7 * units : 7 * units + 2], refs[7 * units + 2 :]
    own, part, w_own = (refs[i * units : (i + 1) * units] for i in range(3))
    own_sem, state_sem, push_send, push_recv, ring_send, ring_recv, pass_send, pass_recv, first_recv, tail_recv = refs[3 * units :]

    me = lax.axis_index("dp")
    z, core = me // CORES, me % CORES
    ring = n // CORES
    partner = z * CORES + 1 - core
    last = ring - 1
    ways = (0, 1)
    lead, *others = order

    def chip(offset):
        return lax.rem(z + offset + 2 * ring, ring)

    def behind(d, j):
        return chip(j if d else -j)

    def owner(d, k):
        return behind(d, k + 1)

    def to(index):
        return {"device_id": {"dp": index}, "device_id_type": pl.DeviceIdType.MESH}

    def following(d):
        return to(behind(d, -1) * CORES + core)

    def wait_bytes(ref, sem):
        pltpu.make_async_copy(ref, ref, sem).wait()

    def load_own(k, u):
        slot = lax.rem(k, 2)
        for d in ways:
            pltpu.make_async_copy(g[u].at[d, owner(d, k) * CORES + core], own[u].at[slot, d], own_sem.at[slot, u]).start()

    def push(d, k, u, sem, rows=slice(None)):
        pltpu.make_async_remote_copy(
            g[u].at[d, owner(d, k) * CORES + 1 - core, rows], part[u].at[d, k, rows], push_send.at[d, u], sem, **to(partner)
        ).start()

    def push_all(k, u):
        for d in ways:
            push(d, k, u, push_recv.at[k, u])

    def terms_here(k, u):
        wait_bytes(own[u].at[lax.rem(k, 2)], own_sem.at[lax.rem(k, 2), u])
        wait_bytes(part[u].at[:, k], push_recv.at[k, u])

    def send(block, d, t, u, rows=slice(None), sem=None):
        piece = out[u].at[d, block, rows]
        sem = ring_recv.at[lax.rem(t, 3), d, u] if sem is None else sem
        pltpu.make_async_remote_copy(piece, piece, ring_send.at[d, u], sem, **following(d)).start()

    def sent(d, u):
        wait_bytes(out[u].at[d, 0], ring_send.at[d, u])

    def arrived(block, d, t, u):
        wait_bytes(out[u].at[d, block], ring_recv.at[lax.rem(t, 3), d, u])

    def pass_on(block, d, u, rows=slice(None)):
        piece = out[u].at[d, block, rows]
        pltpu.make_async_remote_copy(piece, piece, pass_send.at[d, u], pass_recv.at[d, u], **to(partner)).start()

    def terms(slot, d, k, u, row):
        return own[u][slot, d, row].astype(jnp.float32) + part[u][d, k, row].astype(jnp.float32)

    rows_of = [x.shape[2] for x in own]

    for u in order:
        load_own(0, u)

    barrier = pltpu.get_barrier_semaphore()
    for index in (chip(1) * CORES + core, chip(-1) * CORES + core, partner):
        pl.semaphore_signal(barrier, inc=1, **to(index))
    pl.semaphore_wait(barrier, 3)

    for p, (at, count) in enumerate(cuts(rows_of[lead])):
        for d in ways:
            push(d, 0, lead, first_recv.at[d, p], pl.ds(at, count))
    for u in others:
        push_all(0, u)
    for u in order:
        load_own(1, u)
        push_all(1, u)

    def begin(d, u, at, count):
        block = owner(d, 0) * CORES + core

        @pl.loop(at, at + count)
        def _(row):
            out[u][d, block, row] = terms(0, d, 0, u, row).astype(out[u].dtype)

        send(block, d, 0, u, pl.ds(at, count))

    wait_bytes(own[lead].at[0], own_sem.at[0, lead])
    for p, (at, count) in enumerate(cuts(rows_of[lead])):
        for d in ways:
            wait_bytes(part[lead].at[d, 0, pl.ds(at, count)], first_recv.at[d, p])
            begin(d, lead, at, count)
    for u in others:
        terms_here(0, u)
        for d in ways:
            begin(d, u, 0, rows_of[u])

    state = {}
    for u in order:
        state[u] = (
            pltpu.make_async_copy(w[u].at[:, me], w_own[u], state_sem.at[0, u]),
            pltpu.make_async_copy(m_in[u], m[u], state_sem.at[1, u]),
            pltpu.make_async_copy(v_in[u], v[u], state_sem.at[2, u]),
        )
        for copy in state[u]:
            copy.start()

    @pl.loop(1, last)
    def _(k):
        slot = lax.rem(k, 2)
        for u in order:
            load_own(k + 1, u)
            push_all(k + 1, u)
        for u in order:
            terms_here(k, u)
            for d in ways:
                block = owner(d, k) * CORES + core
                arrived(block, d, k - 1, u)

                @pl.loop(0, rows_of[u])
                def _(row):
                    total = out[u][d, block, row].astype(jnp.float32) + terms(slot, d, k, u, row)
                    out[u][d, block, row] = total.astype(out[u].dtype)

                sent(d, u)
                send(block, d, k, u)

    for u in order:
        terms_here(last, u)
        for copy in state[u]:
            copy.wait()
        for d in ways:
            arrived(me, d, last - 1, u)

            @pl.loop(0, rows_of[u])
            def _(row):
                total = out[u][d, me, row].astype(jnp.float32) + terms(last % 2, d, last, u, row)
                gradient = total.astype(jnp.bfloat16).astype(jnp.float32)
                new = adamw(w_own[u][d, row].astype(jnp.float32), m[u][d, row], v[u][d, row], gradient)
                out[u][d, me, row], m[u][d, row], v[u][d, row] = new

            sent(d, u)
            send(me, d, last, u)
            pass_on(me, d, u)

    @pl.loop(1, last - 1)
    def _(j):
        for u in order:
            for d in ways:
                block = behind(d, j) * CORES + core
                arrived(block, d, last + j - 1, u)
                sent(d, u)
                send(block, d, last + j, u)
                pass_on(block, d, u)

    for u in order:
        for d in ways:
            block = behind(d, last - 1) * CORES + core
            arrived(block, d, 2 * last - 2, u)
            if u in late:

                @pl.loop(0, rows_of[u])
                def _(row):
                    after[d][late.index(u), row] = out[u][d, block, row]

            else:
                sent(d, u)
                for p, (at, count) in enumerate(cuts(rows_of[u])[::-1]):
                    send(block, d, 2 * last - 1, u, pl.ds(at, count), tail_recv.at[d, p])
            pass_on(block, d, u)

    for p, (at, count) in enumerate(cuts(rows_of[lead])[::-1]):
        for d in ways:
            block = behind(d, last) * CORES + core
            wait_bytes(out[lead].at[d, block, pl.ds(at, count)], tail_recv.at[d, p])
            pass_on(block, d, lead, pl.ds(at, count))

    for u in order:
        for d in ways:
            sent(d, u)
            wait_bytes(part[u].at[d], push_send.at[d, u])
            passed = out[u].at[d, pl.ds(0, last if u in late else ring)]
            wait_bytes(passed, pass_send.at[d, u])
            wait_bytes(passed, pass_recv.at[d, u])


def place(*refs):
    count = (len(refs) - 1) // 2
    copies = [pltpu.make_async_copy(refs[i], refs[count + i], refs[-1].at[i]) for i in range(count)]
    for copy in copies:
        copy.start()
    for copy in copies:
        copy.wait()


def put(n, late, *refs):
    blocks, out, sem = refs[len(late) : len(late) + 4], refs[len(late) + 4 : 2 * len(late) + 4], refs[-1]
    me = lax.axis_index("dp")
    z, core = me // CORES, me % CORES
    ring = n // CORES
    copies = []
    for d in range(2):
        block = lax.rem(z + (ring - 1 if d else 1), ring) * CORES
        for i in range(len(late)):
            for which, index in ((0, block + core), (2, block + 1 - core)):
                copies.append(pltpu.make_async_copy(blocks[which + d].at[i], out[i].at[d, index], sem.at[len(copies)]))
    for copy in copies:
        copy.start()
    for copy in copies:
        copy.wait()


def solution(mesh):
    n = mesh.shape["dp"]

    def step(*arrays):
        terms, weights, m, v = (arrays[i : i + 3] for i in (0, 3, 6, 9))
        units = len(terms)
        order, late = (2, 0, 1), (0, 1)
        layers = weights[0].shape[0]

        def blocks(x, count):
            return x.reshape(layers, *([count] if count else []), -1, SUBLANES, x.shape[-1])

        terms = [blocks(t[0], n) for t in terms]
        weights_in = [blocks(x, n) for x in weights]
        m_in = [blocks(x, 0) for x in m]
        v_in = [blocks(x, 0) for x in v]
        ring = n // CORES
        block = [x.shape[1:] for x in m_in]
        dma = lambda *shape: pltpu.SemaphoreType.DMA(shape)
        new = pl.pallas_call(
            functools.partial(kernel, n, order, late),
            out_shape=[
                *(pltpu.VMEM(x.shape, x.dtype) for x in (*weights_in, *m_in, *v_in)),
                *[pltpu.VMEM((len(late), *block[late[0]]), jnp.bfloat16)] * 2,
            ],
            in_specs=[pl.BlockSpec(memory_space=pltpu.HBM)] * (4 * units),
            out_specs=[pl.BlockSpec(memory_space=pltpu.VMEM)] * (3 * units + 2),
            scratch_shapes=[
                *(pltpu.VMEM((2, 2, *b), jnp.bfloat16) for b in block),
                *(pltpu.VMEM((2, ring, *b), jnp.bfloat16) for b in block),
                *(pltpu.VMEM((2, *b), jnp.bfloat16) for b in block),
                dma(2, units),
                dma(3, units),
                dma(2, units),
                dma(ring, units),
                dma(2, units),
                dma(3, 2, units),
                dma(2, units),
                dma(2, units),
                dma(2, 3),
                dma(2, 3),
            ],
            compiler_params=pltpu.CompilerParams(collective_id=0, has_side_effects=True, vmem_limit_bytes=VMEM_LIMIT),
            name="step_end",
        )(*(pltpu.with_memory_space_constraint(x, pltpu.HBM) for x in (*terms, *weights_in, *m_in, *v_in)))
        new, after = new[: 3 * units], new[3 * units :]
        far = [lax.ppermute(x, "dp", [(i, (i + way * CORES) % n) for i in range(n)]) for x, way in zip(after, (1, -1), strict=True)]
        new = pl.pallas_call(
            place,
            out_shape=[jax.ShapeDtypeStruct(x.shape, x.dtype) for x in new],
            in_specs=[pl.BlockSpec(memory_space=pltpu.VMEM)] * len(new),
            out_specs=[pl.BlockSpec(memory_space=pltpu.HBM)] * len(new),
            scratch_shapes=[dma(len(new))],
            compiler_params=pltpu.CompilerParams(vmem_limit_bytes=VMEM_LIMIT),
            name="place",
            cost_estimate=pl.CostEstimate(flops=3 * 10**9, bytes_accessed=4 * 10**7, transcendentals=0),
        )(*(pltpu.with_memory_space_constraint(x, pltpu.VMEM) for x in new))
        new = list(new)
        *far, new[late[0]] = lax.optimization_barrier((*far, new[late[0]]))
        near = [lax.ppermute(x, "dp", [(i, i ^ 1) for i in range(n)]) for x in far]
        done = pl.pallas_call(
            functools.partial(put, n, late),
            out_shape=[jax.ShapeDtypeStruct(new[u].shape, new[u].dtype) for u in late],
            in_specs=[pl.BlockSpec(memory_space=pltpu.HBM)] * len(late) + [pl.BlockSpec(memory_space=pltpu.VMEM)] * 4,
            out_specs=[pl.BlockSpec(memory_space=pltpu.HBM)] * len(late),
            scratch_shapes=[dma(4 * len(late))],
            input_output_aliases={i: i for i in range(len(late))},
            compiler_params=pltpu.CompilerParams(vmem_limit_bytes=VMEM_LIMIT),
            name="put",
        )(*(new[u] for u in late), *(pltpu.with_memory_space_constraint(x, pltpu.VMEM) for x in (*far, *near)))
        for u, x in zip(late, done, strict=True):
            new[u] = x
        return tuple(x.reshape(like.shape) for x, like in zip(new, (*weights, *m, *v), strict=True))

    all_of, cut = P(None, None, None), P(None, "dp", None)
    return jax.shard_map(
        step,
        mesh=mesh,
        in_specs=(P(("rep", "dp"), None, None, None),) * 3 + (all_of,) * 3 + (cut,) * 6,
        out_specs=(P("rep", None, None),) * 3 + (P("rep", "dp", None),) * 6,
        check_vma=False,
    )
```

```python
import functools

import jax
import jax.numpy as jnp
from jax import lax
from jax.experimental import pallas as pl
from jax.experimental.pallas import tpu as pltpu
from jax.sharding import PartitionSpec as P

CORES = 2
SUBLANES = 8
VMEM_LIMIT = 20 * 2**20


def adamw(w, m, v, g):
    m = 0.9 * m + 0.1 * g
    v = 0.95 * v + 0.05 * g * g
    step = m * lax.rsqrt(v + 1e-8) + 0.1 * w
    return (w - 0.02 * step).astype(jnp.bfloat16), m, v


def cuts(rows):
    a = max(rows // 8, 1)
    b = max(rows // 3, a + 1)
    return (0, a), (a, b - a), (b, rows - b)


def kernel(n, order, late, *refs):
    units = len(order)
    g, w, m_in, v_in, out, m, v = (refs[i * units : (i + 1) * units] for i in range(7))
    after, refs = refs[7 * units : 7 * units + 2], refs[7 * units + 2 :]
    own, part, w_own = (refs[i * units : (i + 1) * units] for i in range(3))
    own_sem, state_sem, push_send, push_recv, ring_send, ring_recv, pass_send, pass_recv, first_recv = refs[3 * units :]

    me = lax.axis_index("dp")
    z, core = me // CORES, me % CORES
    ring = n // CORES
    partner = z * CORES + 1 - core
    last = ring - 1
    ways = (0, 1)
    lead, *others = order
    tail = order[-1]

    def chip(offset):
        return lax.rem(z + offset + 2 * ring, ring)

    def behind(d, j):
        return chip(j if d else -j)

    def owner(d, k):
        return behind(d, k + 1)

    def to(index):
        return {"device_id": {"dp": index}, "device_id_type": pl.DeviceIdType.MESH}

    def following(d):
        return to(behind(d, -1) * CORES + core)

    def wait_bytes(ref, sem):
        pltpu.make_async_copy(ref, ref, sem).wait()

    def load_own(k, u):
        slot = lax.rem(k, 2)
        for d in ways:
            pltpu.make_async_copy(g[u].at[d, owner(d, k) * CORES + core], own[u].at[slot, d], own_sem.at[slot, u]).start()

    def push(d, k, u, sem, rows=slice(None)):
        pltpu.make_async_remote_copy(
            g[u].at[d, owner(d, k) * CORES + 1 - core, rows], part[u].at[d, k, rows], push_send.at[d, u], sem, **to(partner)
        ).start()

    def push_all(k, u):
        for d in ways:
            push(d, k, u, push_recv.at[k, u])

    def terms_here(k, u):
        wait_bytes(own[u].at[lax.rem(k, 2)], own_sem.at[lax.rem(k, 2), u])
        wait_bytes(part[u].at[:, k], push_recv.at[k, u])

    def send(block, d, t, u, rows=slice(None), sem=None):
        piece = out[u].at[d, block, rows]
        sem = ring_recv.at[lax.rem(t, 3), d, u] if sem is None else sem
        pltpu.make_async_remote_copy(piece, piece, ring_send.at[d, u], sem, **following(d)).start()

    def sent(d, u):
        wait_bytes(out[u].at[d, 0], ring_send.at[d, u])

    def arrived(block, d, t, u):
        wait_bytes(out[u].at[d, block], ring_recv.at[lax.rem(t, 3), d, u])

    def pass_on(block, d, u, rows=slice(None)):
        piece = out[u].at[d, block, rows]
        pltpu.make_async_remote_copy(piece, piece, pass_send.at[d, u], pass_recv.at[d, u], **to(partner)).start()

    def terms(slot, d, k, u, row):
        return own[u][slot, d, row].astype(jnp.float32) + part[u][d, k, row].astype(jnp.float32)

    rows_of = [x.shape[2] for x in own]

    for u in order:
        load_own(0, u)

    barrier = pltpu.get_barrier_semaphore()
    for index in (chip(1) * CORES + core, chip(-1) * CORES + core, partner):
        pl.semaphore_signal(barrier, inc=1, **to(index))
    pl.semaphore_wait(barrier, 3)

    for p, (at, count) in enumerate(cuts(rows_of[lead])):
        for d in ways:
            push(d, 0, lead, first_recv.at[d, p], pl.ds(at, count))
    for u in others:
        push_all(0, u)
    for u in order:
        load_own(1, u)
        push_all(1, u)

    def begin(d, u, at, count):
        block = owner(d, 0) * CORES + core

        @pl.loop(at, at + count)
        def _(row):
            out[u][d, block, row] = terms(0, d, 0, u, row).astype(out[u].dtype)

        send(block, d, 0, u, pl.ds(at, count))

    wait_bytes(own[lead].at[0], own_sem.at[0, lead])
    for p, (at, count) in enumerate(cuts(rows_of[lead])):
        for d in ways:
            wait_bytes(part[lead].at[d, 0, pl.ds(at, count)], first_recv.at[d, p])
            begin(d, lead, at, count)
    for u in others:
        terms_here(0, u)
        for d in ways:
            begin(d, u, 0, rows_of[u])

    state = {}
    for u in order:
        state[u] = (
            pltpu.make_async_copy(w[u].at[:, me], w_own[u], state_sem.at[0, u]),
            pltpu.make_async_copy(m_in[u], m[u], state_sem.at[1, u]),
            pltpu.make_async_copy(v_in[u], v[u], state_sem.at[2, u]),
        )
        for copy in state[u]:
            copy.start()

    @pl.loop(1, last)
    def _(k):
        slot = lax.rem(k, 2)
        for u in order:
            load_own(k + 1, u)
            push_all(k + 1, u)
        for u in order:
            terms_here(k, u)
            for d in ways:
                block = owner(d, k) * CORES + core
                arrived(block, d, k - 1, u)

                @pl.loop(0, rows_of[u])
                def _(row):
                    total = out[u][d, block, row].astype(jnp.float32) + terms(slot, d, k, u, row)
                    out[u][d, block, row] = total.astype(out[u].dtype)

                sent(d, u)
                send(block, d, k, u)

    for u in order:
        terms_here(last, u)
        for copy in state[u]:
            copy.wait()
        for d in ways:
            arrived(me, d, last - 1, u)

            @pl.loop(0, rows_of[u])
            def _(row):
                total = out[u][d, me, row].astype(jnp.float32) + terms(last % 2, d, last, u, row)
                gradient = total.astype(jnp.bfloat16).astype(jnp.float32)
                new = adamw(w_own[u][d, row].astype(jnp.float32), m[u][d, row], v[u][d, row], gradient)
                out[u][d, me, row], m[u][d, row], v[u][d, row] = new

            sent(d, u)
            send(me, d, last, u)
            pass_on(me, d, u)

    def forward(d, j, u):
        block = behind(d, j) * CORES + core
        arrived(block, d, last + j - 1, u)
        sent(d, u)
        send(block, d, last + j, u)
        pass_on(block, d, u)

    @pl.loop(1, last - 2)
    def _(j):
        for u in order:
            for d in ways:
                forward(d, j, u)

    for u in order:
        if u == tail:
            for d in ways:
                forward(d, last - 1, lead)
        for d in ways:
            forward(d, last - 2, u)

    for u in others:
        if u == tail:
            for d in ways:
                block = behind(d, last) * CORES + core
                arrived(block, d, 2 * last - 1, lead)
                pass_on(block, d, lead)
        for d in ways:
            block = behind(d, last - 1) * CORES + core
            arrived(block, d, 2 * last - 2, u)

            @pl.loop(0, rows_of[u])
            def _(row):
                after[d][late.index(u), row] = out[u][d, block, row]

    for u in order:
        for d in ways:
            sent(d, u)
            wait_bytes(part[u].at[d], push_send.at[d, u])
            passed = out[u].at[d, pl.ds(0, last - 1 if u in late else ring)]
            wait_bytes(passed, pass_send.at[d, u])
            wait_bytes(passed, pass_recv.at[d, u])


def place(*refs):
    count = (len(refs) - 1) // 2
    copies = [pltpu.make_async_copy(refs[i], refs[count + i], refs[-1].at[i]) for i in range(count)]
    for copy in copies:
        copy.start()
    for copy in copies:
        copy.wait()


def put(n, late, where, *refs):
    count = len(late)
    blocks, out, sem = refs[count : count + len(where)], refs[count + len(where) : -1], refs[-1]
    me = lax.axis_index("dp")
    z, core = me // CORES, me % CORES
    ring = n // CORES
    copies = []
    for part, (d, back, partners) in zip(blocks, where, strict=True):
        index = lax.rem(z + (back if d else ring - back), ring) * CORES + (1 - core if partners else core)
        copies += [pltpu.make_async_copy(part.at[i], out[i].at[d, index], sem.at[len(copies) + i]) for i in range(count)]
    for copy in copies:
        copy.start()
    for copy in copies:
        copy.wait()


def solution(mesh):
    n = mesh.shape["dp"]

    def step(*arrays):
        terms, weights, m, v = (arrays[i : i + 3] for i in (0, 3, 6, 9))
        units = len(terms)
        order, late = (2, 0, 1), (0, 1)
        layers = weights[0].shape[0]

        def blocks(x, count):
            return x.reshape(layers, *([count] if count else []), -1, SUBLANES, x.shape[-1])

        terms = [blocks(t[0], n) for t in terms]
        weights_in = [blocks(x, n) for x in weights]
        m_in = [blocks(x, 0) for x in m]
        v_in = [blocks(x, 0) for x in v]
        ring = n // CORES
        block = [x.shape[1:] for x in m_in]
        dma = lambda *shape: pltpu.SemaphoreType.DMA(shape)
        new = pl.pallas_call(
            functools.partial(kernel, n, order, late),
            out_shape=[
                *(pltpu.VMEM(x.shape, x.dtype) for x in (*weights_in, *m_in, *v_in)),
                *[pltpu.VMEM((len(late), *block[late[0]]), jnp.bfloat16)] * 2,
            ],
            in_specs=[pl.BlockSpec(memory_space=pltpu.HBM)] * (4 * units),
            out_specs=[pl.BlockSpec(memory_space=pltpu.VMEM)] * (3 * units + 2),
            scratch_shapes=[
                *(pltpu.VMEM((2, 2, *b), jnp.bfloat16) for b in block),
                *(pltpu.VMEM((2, ring, *b), jnp.bfloat16) for b in block),
                *(pltpu.VMEM((2, *b), jnp.bfloat16) for b in block),
                dma(2, units),
                dma(3, units),
                dma(2, units),
                dma(ring, units),
                dma(2, units),
                dma(3, 2, units),
                dma(2, units),
                dma(2, units),
                dma(2, 3),
            ],
            compiler_params=pltpu.CompilerParams(collective_id=0, has_side_effects=True, vmem_limit_bytes=VMEM_LIMIT),
            name="step_end",
        )(*(pltpu.with_memory_space_constraint(x, pltpu.HBM) for x in (*terms, *weights_in, *m_in, *v_in)))
        new, after = new[: 3 * units], new[3 * units :]
        across = [(i, i ^ 1) for i in range(n)]
        far = [lax.ppermute(x, "dp", [(i, (i + way * CORES) % n) for i in range(n)]) for x, way in zip(after, (1, -1), strict=True)]
        near = [lax.ppermute(x, "dp", across) for x in after]
        new = pl.pallas_call(
            place,
            out_shape=[jax.ShapeDtypeStruct(x.shape, x.dtype) for x in new],
            in_specs=[pl.BlockSpec(memory_space=pltpu.VMEM)] * len(new),
            out_specs=[pl.BlockSpec(memory_space=pltpu.HBM)] * len(new),
            scratch_shapes=[dma(len(new))],
            compiler_params=pltpu.CompilerParams(vmem_limit_bytes=VMEM_LIMIT),
            name="place",
            cost_estimate=pl.CostEstimate(flops=3 * 10**9, bytes_accessed=4 * 10**7, transcendentals=0),
        )(*(pltpu.with_memory_space_constraint(x, pltpu.VMEM) for x in new))
        new = list(new)
        *far, new[late[0]] = lax.optimization_barrier((*far, new[late[0]]))
        last = n // CORES - 1
        for parts, where in (
            ((*far, *near), ((0, last, 0), (1, last, 0), (0, last - 1, 1), (1, last - 1, 1))),
            ([lax.ppermute(x, "dp", across) for x in far], ((0, last, 1), (1, last, 1))),
        ):
            done = pl.pallas_call(
                functools.partial(put, n, late, where),
                out_shape=[jax.ShapeDtypeStruct(new[u].shape, new[u].dtype) for u in late],
                in_specs=[pl.BlockSpec(memory_space=pltpu.HBM)] * len(late) + [pl.BlockSpec(memory_space=pltpu.VMEM)] * len(parts),
                out_specs=[pl.BlockSpec(memory_space=pltpu.HBM)] * len(late),
                scratch_shapes=[dma(len(where) * len(late))],
                input_output_aliases={i: i for i in range(len(late))},
                compiler_params=pltpu.CompilerParams(vmem_limit_bytes=VMEM_LIMIT),
                cost_estimate=pl.CostEstimate(flops=2 * 10**8, bytes_accessed=2 * 10**6, transcendentals=0),
                name="put",
            )(*(new[u] for u in late), *(pltpu.with_memory_space_constraint(x, pltpu.VMEM) for x in parts))
            for u, x in zip(late, done, strict=True):
                new[u] = x
        return tuple(x.reshape(like.shape) for x, like in zip(new, (*weights, *m, *v), strict=True))

    all_of, cut = P(None, None, None), P(None, "dp", None)
    return jax.shard_map(
        step,
        mesh=mesh,
        in_specs=(P(("rep", "dp"), None, None, None),) * 3 + (all_of,) * 3 + (cut,) * 6,
        out_specs=(P("rep", None, None),) * 3 + (P("rep", "dp", None),) * 6,
        check_vma=False,
    )
```

```python
import functools

import jax
import jax.numpy as jnp
from jax import lax
from jax.experimental import pallas as pl
from jax.experimental.pallas import tpu as pltpu
from jax.sharding import PartitionSpec as P


CORES = 2
SUBLANES = 8
VMEM_LIMIT = 20 * 2**20


def adamw(w, m, v, g):
    m = 0.9 * m + 0.1 * g
    v = 0.95 * v + 0.05 * g * g
    step = m * lax.rsqrt(v + 1e-8) + 0.1 * w
    return (w - 0.02 * step).astype(jnp.bfloat16), m, v


def cuts(rows):
    a = max(rows // 8, 1)
    b = max(rows // 3, a + 1)
    return (0, a), (a, b - a), (b, rows - b)


def kernel(n, order, late, *refs):
    units = len(order)
    g, w, m_in, v_in, out, m, v = (refs[i * units : (i + 1) * units] for i in range(7))
    after, refs = refs[7 * units : 7 * units + 2], refs[7 * units + 2 :]
    own, part, w_own = (refs[i * units : (i + 1) * units] for i in range(3))
    own_sem, state_sem, across_send, push_recv, ring_send, ring_recv, pass_recv, first_recv = refs[3 * units :]

    me = lax.axis_index("dp")
    z, core = me // CORES, me % CORES
    ring = n // CORES
    partner = z * CORES + 1 - core
    last = ring - 1
    ways = (0, 1)
    lead, *others = order
    tail = order[-1]

    def chip(offset):
        return lax.rem(z + offset + 2 * ring, ring)

    def behind(d, j):
        return chip(j if d else -j)

    def owner(d, k):
        return behind(d, k + 1)

    def to(index):
        return {"device_id": {"dp": index}, "device_id_type": pl.DeviceIdType.MESH}

    def following(d):
        return to(behind(d, -1) * CORES + core)

    def wait_bytes(ref, sem):
        pltpu.make_async_copy(ref, ref, sem).wait()

    def load_own(k, u):
        slot = lax.rem(k, 2)
        for d in ways:
            pltpu.make_async_copy(g[u].at[d, owner(d, k) * CORES + core], own[u].at[slot, d], own_sem.at[slot, u]).start()

    def push(d, k, u, sem, rows=slice(None)):
        pltpu.make_async_remote_copy(
            g[u].at[d, owner(d, k) * CORES + 1 - core, rows], part[u].at[d, k, rows], across_send.at[u], sem, **to(partner)
        ).start()

    def push_all(k, u):
        for d in ways:
            push(d, k, u, push_recv.at[k, u])

    def terms_here(k, u):
        wait_bytes(own[u].at[lax.rem(k, 2)], own_sem.at[lax.rem(k, 2), u])
        wait_bytes(part[u].at[:, k], push_recv.at[k, u])

    def send(block, d, t, u, rows=slice(None), sem=None):
        piece = out[u].at[d, block, rows]
        sem = ring_recv.at[lax.rem(t, 3), d, u] if sem is None else sem
        pltpu.make_async_remote_copy(piece, piece, ring_send.at[u], sem, **following(d)).start()

    def sent(u):
        wait_bytes(out[u].at[:, 0], ring_send.at[u])

    def arrived(block, d, t, u):
        wait_bytes(out[u].at[d, block], ring_recv.at[lax.rem(t, 3), d, u])

    def pass_on(block, d, u, rows=slice(None)):
        piece = out[u].at[d, block, rows]
        pltpu.make_async_remote_copy(piece, piece, across_send.at[u], pass_recv.at[u], **to(partner)).start()

    def terms(slot, d, k, u, row):
        return own[u][slot, d, row].astype(jnp.float32) + part[u][d, k, row].astype(jnp.float32)

    rows_of = [x.shape[2] for x in own]

    for u in order:
        load_own(0, u)

    barrier = pltpu.get_barrier_semaphore()
    for index in (chip(1) * CORES + core, chip(-1) * CORES + core, partner):
        pl.semaphore_signal(barrier, inc=1, **to(index))
    pl.semaphore_wait(barrier, 3)

    for p, (at, count) in enumerate(cuts(rows_of[lead])):
        for d in ways:
            push(d, 0, lead, first_recv.at[d, p], pl.ds(at, count))
    for u in others:
        push_all(0, u)
    for u in order:
        load_own(1, u)
        push_all(1, u)

    def begin(d, u, at, count):
        block = owner(d, 0) * CORES + core

        @pl.loop(at, at + count)
        def _(row):
            out[u][d, block, row] = terms(0, d, 0, u, row).astype(out[u].dtype)

        send(block, d, 0, u, pl.ds(at, count))

    wait_bytes(own[lead].at[0], own_sem.at[0, lead])
    for p, (at, count) in enumerate(cuts(rows_of[lead])):
        for d in ways:
            wait_bytes(part[lead].at[d, 0, pl.ds(at, count)], first_recv.at[d, p])
            begin(d, lead, at, count)
    for u in others:
        terms_here(0, u)
        for d in ways:
            begin(d, u, 0, rows_of[u])

    state = {}
    for u in order:
        state[u] = (
            pltpu.make_async_copy(w[u].at[:, me], w_own[u], state_sem.at[0, u]),
            pltpu.make_async_copy(m_in[u], m[u], state_sem.at[1, u]),
            pltpu.make_async_copy(v_in[u], v[u], state_sem.at[2, u]),
        )
        for copy in state[u]:
            copy.start()

    @pl.loop(1, last)
    def _(k):
        slot = lax.rem(k, 2)
        for u in order:
            load_own(k + 1, u)
            push_all(k + 1, u)
        for u in order:
            terms_here(k, u)
            for d in ways:
                block = owner(d, k) * CORES + core
                arrived(block, d, k - 1, u)

                @pl.loop(0, rows_of[u])
                def _(row):
                    total = out[u][d, block, row].astype(jnp.float32) + terms(slot, d, k, u, row)
                    out[u][d, block, row] = total.astype(out[u].dtype)

                if d == 0:
                    sent(u)
                send(block, d, k, u)

    for u in order:
        terms_here(last, u)
        for copy in state[u]:
            copy.wait()
        for d in ways:
            arrived(me, d, last - 1, u)

            @pl.loop(0, rows_of[u])
            def _(row):
                total = out[u][d, me, row].astype(jnp.float32) + terms(last % 2, d, last, u, row)
                gradient = total.astype(jnp.bfloat16).astype(jnp.float32)
                new = adamw(w_own[u][d, row].astype(jnp.float32), m[u][d, row], v[u][d, row], gradient)
                out[u][d, me, row], m[u][d, row], v[u][d, row] = new

            if d == 0:
                sent(u)
            send(me, d, last, u)
            pass_on(me, d, u)

    def forward(d, j, u):
        block = behind(d, j) * CORES + core
        arrived(block, d, last + j - 1, u)
        if d == 0:
            sent(u)
        send(block, d, last + j, u)
        pass_on(block, d, u)

    @pl.loop(1, last - 2)
    def _(j):
        for u in order:
            for d in ways:
                forward(d, j, u)

    for u in order:
        if u == tail:
            for d in ways:
                forward(d, last - 1, lead)
        for d in ways:
            forward(d, last - 2, u)

    for u in others:
        if u == tail:
            for d in ways:
                block = behind(d, last) * CORES + core
                arrived(block, d, 2 * last - 1, lead)
                pass_on(block, d, lead)
        for d in ways:
            block = behind(d, last - 1) * CORES + core
            arrived(block, d, 2 * last - 2, u)

            @pl.loop(0, rows_of[u])
            def _(row):
                after[d][late.index(u), row] = out[u][d, block, row]

    for u in order:
        sent(u)
        passed = last - 1 if u in late else ring
        wait_bytes(out[u].at[:, pl.ds(0, ring + passed)], across_send.at[u])
        wait_bytes(out[u].at[:, pl.ds(0, passed)], pass_recv.at[u])


def place(*refs):
    count = (len(refs) - 1) // 2
    copies = [pltpu.make_async_copy(refs[i], refs[count + i], refs[-1].at[i]) for i in range(count)]
    for copy in copies:
        copy.start()
    for copy in copies:
        copy.wait()


def put(n, late, where, *refs):
    count = len(late)
    blocks, out, sem = refs[count : count + len(where)], refs[-1 - count : -1], refs[-1]
    me = lax.axis_index("dp")
    z, core = me // CORES, me % CORES
    ring = n // CORES
    copies = []
    for part, (d, back, partners) in zip(blocks, where, strict=True):
        index = lax.rem(z + (back if d else ring - back), ring) * CORES + (1 - core if partners else core)
        copies += [pltpu.make_async_copy(part.at[i], out[i].at[d, index], sem.at[len(copies) + i]) for i in range(count)]
    for copy in copies:
        copy.start()
    for copy in copies:
        copy.wait()


def marker(ref, out):
    out[...] = jnp.zeros_like(out)


def solution(mesh):
    n = mesh.shape["dp"]

    def step(*arrays):
        return whole_step(*arrays)

    def whole_step(*arrays):
        terms, weights, m, v = (arrays[i : i + 3] for i in (0, 3, 6, 9))
        units = len(terms)
        order, late = (2, 0, 1), (0, 1)
        layers = weights[0].shape[0]

        def blocks(x, count):
            return x.reshape(layers, *([count] if count else []), -1, SUBLANES, x.shape[-1])

        terms = [blocks(t[0], n) for t in terms]
        weights_in = [blocks(x, n) for x in weights]
        m_in = [blocks(x, 0) for x in m]
        v_in = [blocks(x, 0) for x in v]
        ring = n // CORES
        block = [x.shape[1:] for x in m_in]
        dma = lambda *shape: pltpu.SemaphoreType.DMA(shape)
        new = pl.pallas_call(
            functools.partial(kernel, n, order, late),
            out_shape=[
                *(pltpu.VMEM(x.shape, x.dtype) for x in (*weights_in, *m_in, *v_in)),
                *[pltpu.VMEM((len(late), *block[late[0]]), jnp.bfloat16)] * 2,
            ],
            in_specs=[pl.BlockSpec(memory_space=pltpu.HBM)] * (4 * units),
            out_specs=[pl.BlockSpec(memory_space=pltpu.VMEM)] * (3 * units + 2),
            scratch_shapes=[
                *(pltpu.VMEM((2, 2, *b), jnp.bfloat16) for b in block),
                *(pltpu.VMEM((2, ring, *b), jnp.bfloat16) for b in block),
                *(pltpu.VMEM((2, *b), jnp.bfloat16) for b in block),
                dma(2, units),
                dma(3, units),
                dma(units),
                dma(ring, units),
                dma(units),
                dma(3, 2, units),
                dma(units),
                dma(2, 3),
            ],
            compiler_params=pltpu.CompilerParams(collective_id=0, has_side_effects=True, vmem_limit_bytes=VMEM_LIMIT),
            name="step_end",
        )(*(pltpu.with_memory_space_constraint(x, pltpu.HBM) for x in (*terms, *weights_in, *m_in, *v_in)))
        new, after = new[: 3 * units], new[3 * units :]
        across = [(i, i ^ 1) for i in range(n)]
        far = []
        for d, way in enumerate((1, -1)):
            far.append(lax.ppermute(after[d], "dp", [(i, (i + way * CORES) % n) for i in range(n)]))
        near = [lax.ppermute(x, "dp", across) for x in after]
        writer = pl.pallas_call(
            place,
            out_shape=[jax.ShapeDtypeStruct(x.shape, x.dtype) for x in new],
            in_specs=[pl.BlockSpec(memory_space=pltpu.VMEM)] * len(new),
            out_specs=[pl.BlockSpec(memory_space=pltpu.HBM)] * len(new),
            scratch_shapes=[dma(len(new))],
            compiler_params=pltpu.CompilerParams(vmem_limit_bytes=VMEM_LIMIT),
            name="place",
            cost_estimate=pl.CostEstimate(flops=3 * 10**9, bytes_accessed=4 * 10**7, transcendentals=0),
        )
        new = list(writer(*(pltpu.with_memory_space_constraint(x, pltpu.VMEM) for x in new)))
        last = n // CORES - 1

        def write(parts, where):
            done = pl.pallas_call(
                functools.partial(put, n, late, where),
                out_shape=[jax.ShapeDtypeStruct(new[u].shape, new[u].dtype) for u in late],
                in_specs=[pl.BlockSpec(memory_space=pltpu.HBM)] * len(late) + [pl.BlockSpec(memory_space=pltpu.VMEM)] * len(parts),
                out_specs=[pl.BlockSpec(memory_space=pltpu.HBM)] * len(late),
                scratch_shapes=[dma(len(where) * len(late))],
                input_output_aliases={i: i for i in range(len(late))},
                compiler_params=pltpu.CompilerParams(vmem_limit_bytes=VMEM_LIMIT),
                cost_estimate=pl.CostEstimate(flops=2 * 10**8, bytes_accessed=2 * 10**6, transcendentals=0),
                name="put",
            )(*(new[u] for u in late), *(pltpu.with_memory_space_constraint(x, pltpu.VMEM) for x in parts))
            for u, x in zip(late, done, strict=True):
                new[u] = x

        def swap(d):
            far[d], new[late[0]] = lax.optimization_barrier((far[d], new[late[0]]))
            return lax.ppermute(far[d], "dp", across)

        swapped = {1: swap(1)}
        mark = pl.pallas_call(
            marker,
            out_shape=pltpu.VMEM((SUBLANES, 128), jnp.float32),
            in_specs=[pl.BlockSpec(memory_space=pltpu.VMEM)],
            out_specs=pl.BlockSpec(memory_space=pltpu.VMEM),
            compiler_params=pltpu.CompilerParams(vmem_limit_bytes=VMEM_LIMIT),
            cost_estimate=pl.CostEstimate(flops=10**5, bytes_accessed=10**4, transcendentals=0),
            name="mark",
        )(far[1])
        far[0], mark = lax.optimization_barrier((far[0], mark))
        swapped[0] = swap(0)
        write((*far, *near, mark), ((0, last, 0), (1, last, 0), (0, last - 1, 1), (1, last - 1, 1)))
        write((swapped[0], swapped[1]), ((0, last, 1), (1, last, 1)))
        return tuple(x.reshape(like.shape) for x, like in zip(new, (*weights, *m, *v), strict=True))

    all_of, cut = P(None, None, None), P(None, "dp", None)
    step = jax.shard_map(
        step,
        mesh=mesh,
        in_specs=(P(("rep", "dp"), None, None, None),) * 3 + (all_of,) * 3 + (cut,) * 6,
        out_specs=(P("rep", None, None),) * 3 + (P("rep", "dp", None),) * 6,
        check_vma=False,
    )
    return step
```

```python
import functools

import jax
import jax.numpy as jnp
from jax import lax
from jax.experimental import pallas as pl
from jax.experimental.pallas import tpu as pltpu
from jax.sharding import PartitionSpec as P


CORES = 2
SUBLANES = 8
VMEM_LIMIT = 20 * 2**20


def adamw(w, m, v, g):
    m = 0.9 * m + 0.1 * g
    v = 0.95 * v + 0.05 * g * g
    step = m * lax.rsqrt(v + 1e-8) + 0.1 * w
    return (w - 0.02 * step).astype(jnp.bfloat16), m, v


def cuts(rows):
    a = max(rows // 8, 1)
    b = max(rows // 3, a + 1)
    return (0, a), (a, b - a), (b, rows - b)


def kernel(n, order, late, *refs):
    units = len(order)
    g, w, m_in, v_in, out, m, v = (refs[i * units : (i + 1) * units] for i in range(7))
    after, refs = refs[7 * units : 7 * units + 2], refs[7 * units + 2 :]
    own, part, w_own = (refs[i * units : (i + 1) * units] for i in range(3))
    across_send, ring_send, ring_recv, pass_recv = refs[3 * units :]

    me = lax.axis_index("dp")
    z, core = me // CORES, me % CORES
    ring = n // CORES
    partner = z * CORES + 1 - core
    last = ring - 1
    ways = (0, 1)
    lead, *others = order
    tail = order[-1]

    def chip(offset):
        return lax.rem(z + offset + 2 * ring, ring)

    def behind(d, j):
        return chip(j if d else -j)

    def owner(d, k):
        return behind(d, k + 1)

    def to(index):
        return {"device_id": {"dp": index}, "device_id_type": pl.DeviceIdType.MESH}

    def following(d):
        return to(behind(d, -1) * CORES + core)

    def wait_bytes(ref, sem):
        pltpu.make_async_copy(ref, ref, sem).wait()

    def push(d, k, u, sem, rows=slice(None)):
        pltpu.make_async_remote_copy(
            g[u].at[d, owner(d, k) * CORES + 1 - core, rows], part[u].at[d, k, rows], across_send.at[u], sem, **to(partner)
        ).start()

    def send(block, d, t, u, rows=slice(None), sem=None):
        piece = out[u].at[d, block, rows]
        sem = ring_recv.at[lax.rem(t, 3), d, u] if sem is None else sem
        pltpu.make_async_remote_copy(piece, piece, ring_send.at[u], sem, **following(d)).start()

    def sent(u):
        wait_bytes(out[u].at[:, 0], ring_send.at[u])

    def arrived(block, d, t, u):
        wait_bytes(out[u].at[d, block], ring_recv.at[lax.rem(t, 3), d, u])

    def pass_on(block, d, u, rows=slice(None)):
        piece = out[u].at[d, block, rows]
        pltpu.make_async_remote_copy(piece, piece, across_send.at[u], pass_recv.at[u], **to(partner)).start()

    def terms(slot, d, k, u, row):
        return own[u][slot, d, row].astype(jnp.float32) + part[u][d, k, row].astype(jnp.float32)

    rows_of = [x.shape[2] for x in own]

    def sums(own_sem, state_sem, push_recv, first_recv):
        def load_own(k, u):
            slot = lax.rem(k, 2)
            for d in ways:
                pltpu.make_async_copy(g[u].at[d, owner(d, k) * CORES + core], own[u].at[slot, d], own_sem.at[slot, u]).start()

        def push_all(k, u):
            for d in ways:
                push(d, k, u, push_recv.at[k, u])

        def terms_here(k, u):
            wait_bytes(own[u].at[lax.rem(k, 2)], own_sem.at[lax.rem(k, 2), u])
            wait_bytes(part[u].at[:, k], push_recv.at[k, u])

        for u in order:
            load_own(0, u)

        barrier = pltpu.get_barrier_semaphore()
        for index in (chip(1) * CORES + core, chip(-1) * CORES + core, partner):
            pl.semaphore_signal(barrier, inc=1, **to(index))
        pl.semaphore_wait(barrier, 3)

        for p, (at, count) in enumerate(cuts(rows_of[lead])):
            for d in ways:
                push(d, 0, lead, first_recv.at[d, p], pl.ds(at, count))
        for u in others:
            push_all(0, u)
        for u in order:
            load_own(1, u)
            push_all(1, u)

        def begin(d, u, at, count):
            block = owner(d, 0) * CORES + core

            @pl.loop(at, at + count)
            def _(row):
                out[u][d, block, row] = terms(0, d, 0, u, row).astype(out[u].dtype)

            send(block, d, 0, u, pl.ds(at, count))

        wait_bytes(own[lead].at[0], own_sem.at[0, lead])
        for p, (at, count) in enumerate(cuts(rows_of[lead])):
            for d in ways:
                wait_bytes(part[lead].at[d, 0, pl.ds(at, count)], first_recv.at[d, p])
                begin(d, lead, at, count)
        for u in others:
            terms_here(0, u)
            for d in ways:
                begin(d, u, 0, rows_of[u])

        state = {}
        for u in order:
            state[u] = (
                pltpu.make_async_copy(w[u].at[:, me], w_own[u], state_sem.at[0, u]),
                pltpu.make_async_copy(m_in[u], m[u], state_sem.at[1, u]),
                pltpu.make_async_copy(v_in[u], v[u], state_sem.at[2, u]),
            )
            for copy in state[u]:
                copy.start()

        @pl.loop(1, last)
        def _(k):
            slot = lax.rem(k, 2)
            for u in order:
                load_own(k + 1, u)
                push_all(k + 1, u)
            for u in order:
                terms_here(k, u)
                for d in ways:
                    block = owner(d, k) * CORES + core
                    arrived(block, d, k - 1, u)

                    @pl.loop(0, rows_of[u])
                    def _(row):
                        total = out[u][d, block, row].astype(jnp.float32) + terms(slot, d, k, u, row)
                        out[u][d, block, row] = total.astype(out[u].dtype)

                    if d == 0:
                        sent(u)
                    send(block, d, k, u)

        for u in order:
            terms_here(last, u)
            for copy in state[u]:
                copy.wait()
            for d in ways:
                arrived(me, d, last - 1, u)

                @pl.loop(0, rows_of[u])
                def _(row):
                    total = out[u][d, me, row].astype(jnp.float32) + terms(last % 2, d, last, u, row)
                    gradient = total.astype(jnp.bfloat16).astype(jnp.float32)
                    new = adamw(w_own[u][d, row].astype(jnp.float32), m[u][d, row], v[u][d, row], gradient)
                    out[u][d, me, row], m[u][d, row], v[u][d, row] = new

                if d == 0:
                    sent(u)
                send(me, d, last, u)
                pass_on(me, d, u)

    dma = lambda *shape: pltpu.SemaphoreType.DMA(shape)
    pl.run_scoped(sums, dma(2, units), dma(3, units), dma(ring, units), dma(2, len(cuts(rows_of[lead]))))

    def forward(d, j, u):
        block = behind(d, j) * CORES + core
        arrived(block, d, last + j - 1, u)
        if d == 0:
            sent(u)
        send(block, d, last + j, u)
        pass_on(block, d, u)

    @pl.loop(1, last - 2)
    def _(j):
        for u in order:
            for d in ways:
                forward(d, j, u)

    for u in order:
        if u == tail:
            for d in ways:
                forward(d, last - 1, lead)
        for d in ways:
            forward(d, last - 2, u)

    for u in others:
        if u == tail:
            for d in ways:
                block = behind(d, last) * CORES + core
                arrived(block, d, 2 * last - 1, lead)
                pass_on(block, d, lead)
        for d in ways:
            block = behind(d, last - 1) * CORES + core
            arrived(block, d, 2 * last - 2, u)

            @pl.loop(0, rows_of[u])
            def _(row):
                after[d][late.index(u), row] = out[u][d, block, row]

    for u in order:
        sent(u)
        passed = last - 1 if u in late else ring
        wait_bytes(out[u].at[:, pl.ds(0, ring + passed)], across_send.at[u])
        wait_bytes(out[u].at[:, pl.ds(0, passed)], pass_recv.at[u])


def place(*refs):
    count = (len(refs) - 1) // 2
    copies = [pltpu.make_async_copy(refs[i], refs[count + i], refs[-1].at[i]) for i in range(count)]
    for copy in copies:
        copy.start()
    for copy in copies:
        copy.wait()


def put(n, late, where, *refs):
    count = len(late)
    blocks, out, sem = refs[count : count + len(where)], refs[-1 - count : -1], refs[-1]
    me = lax.axis_index("dp")
    z, core = me // CORES, me % CORES
    ring = n // CORES
    copies = []
    for part, (d, back, partners) in zip(blocks, where, strict=True):
        index = lax.rem(z + (back if d else ring - back), ring) * CORES + (1 - core if partners else core)
        copies += [pltpu.make_async_copy(part.at[i], out[i].at[d, index], sem.at[len(copies) + i]) for i in range(count)]
    for copy in copies:
        copy.start()
    for copy in copies:
        copy.wait()


def marker(ref, out):
    out[...] = jnp.zeros_like(out)


def solution(mesh):
    n = mesh.shape["dp"]

    def step(*arrays):
        return whole_step(*arrays)

    def whole_step(*arrays):
        terms, weights, m, v = (arrays[i : i + 3] for i in (0, 3, 6, 9))
        units = len(terms)
        order, late = (2, 0, 1), (0, 1)
        layers = weights[0].shape[0]

        def blocks(x, count):
            return x.reshape(layers, *([count] if count else []), -1, SUBLANES, x.shape[-1])

        terms = [blocks(t[0], n) for t in terms]
        weights_in = [blocks(x, n) for x in weights]
        m_in = [blocks(x, 0) for x in m]
        v_in = [blocks(x, 0) for x in v]
        ring = n // CORES
        block = [x.shape[1:] for x in m_in]
        dma = lambda *shape: pltpu.SemaphoreType.DMA(shape)
        new = pl.pallas_call(
            functools.partial(kernel, n, order, late),
            out_shape=[
                *(pltpu.VMEM(x.shape, x.dtype) for x in (*weights_in, *m_in, *v_in)),
                *[pltpu.VMEM((len(late), *block[late[0]]), jnp.bfloat16)] * 2,
            ],
            in_specs=[pl.BlockSpec(memory_space=pltpu.HBM)] * (4 * units),
            out_specs=[pl.BlockSpec(memory_space=pltpu.VMEM)] * (3 * units + 2),
            scratch_shapes=[
                *(pltpu.VMEM((2, 2, *b), jnp.bfloat16) for b in block),
                *(pltpu.VMEM((2, ring, *b), jnp.bfloat16) for b in block),
                *(pltpu.VMEM((2, *b), jnp.bfloat16) for b in block),
                dma(units),
                dma(units),
                dma(3, 2, units),
                dma(units),
            ],
            compiler_params=pltpu.CompilerParams(collective_id=0, has_side_effects=True, vmem_limit_bytes=VMEM_LIMIT),
            name="step_end",
        )(*(pltpu.with_memory_space_constraint(x, pltpu.HBM) for x in (*terms, *weights_in, *m_in, *v_in)))
        new, after = new[: 3 * units], new[3 * units :]
        across = [(i, i ^ 1) for i in range(n)]
        far = []
        for d, way in enumerate((1, -1)):
            far.append(lax.ppermute(after[d], "dp", [(i, (i + way * CORES) % n) for i in range(n)]))
        near = [lax.ppermute(x, "dp", across) for x in after]
        writer = pl.pallas_call(
            place,
            out_shape=[jax.ShapeDtypeStruct(x.shape, x.dtype) for x in new],
            in_specs=[pl.BlockSpec(memory_space=pltpu.VMEM)] * len(new),
            out_specs=[pl.BlockSpec(memory_space=pltpu.HBM)] * len(new),
            scratch_shapes=[dma(len(new))],
            compiler_params=pltpu.CompilerParams(vmem_limit_bytes=VMEM_LIMIT),
            name="place",
            cost_estimate=pl.CostEstimate(flops=3 * 10**9, bytes_accessed=4 * 10**7, transcendentals=0),
        )
        new = list(writer(*(pltpu.with_memory_space_constraint(x, pltpu.VMEM) for x in new)))
        last = n // CORES - 1

        def write(parts, where):
            done = pl.pallas_call(
                functools.partial(put, n, late, where),
                out_shape=[jax.ShapeDtypeStruct(new[u].shape, new[u].dtype) for u in late],
                in_specs=[pl.BlockSpec(memory_space=pltpu.HBM)] * len(late) + [pl.BlockSpec(memory_space=pltpu.VMEM)] * len(parts),
                out_specs=[pl.BlockSpec(memory_space=pltpu.HBM)] * len(late),
                scratch_shapes=[dma(len(where) * len(late))],
                input_output_aliases={i: i for i in range(len(late))},
                compiler_params=pltpu.CompilerParams(vmem_limit_bytes=VMEM_LIMIT),
                cost_estimate=pl.CostEstimate(flops=2 * 10**8, bytes_accessed=2 * 10**6, transcendentals=0),
                name="put",
            )(*(new[u] for u in late), *(pltpu.with_memory_space_constraint(x, pltpu.VMEM) for x in parts))
            for u, x in zip(late, done, strict=True):
                new[u] = x

        def swap(d):
            far[d], new[late[0]] = lax.optimization_barrier((far[d], new[late[0]]))
            return lax.ppermute(far[d], "dp", across)

        swapped = {1: swap(1)}
        mark = pl.pallas_call(
            marker,
            out_shape=pltpu.VMEM((SUBLANES, 128), jnp.float32),
            in_specs=[pl.BlockSpec(memory_space=pltpu.VMEM)],
            out_specs=pl.BlockSpec(memory_space=pltpu.VMEM),
            compiler_params=pltpu.CompilerParams(vmem_limit_bytes=VMEM_LIMIT),
            cost_estimate=pl.CostEstimate(flops=10**5, bytes_accessed=10**4, transcendentals=0),
            name="mark",
        )(far[1])
        far[0], mark = lax.optimization_barrier((far[0], mark))
        swapped[0] = swap(0)
        write((*far, *near, mark), ((0, last, 0), (1, last, 0), (0, last - 1, 1), (1, last - 1, 1)))
        write((swapped[0], swapped[1]), ((0, last, 1), (1, last, 1)))
        return tuple(x.reshape(like.shape) for x, like in zip(new, (*weights, *m, *v), strict=True))

    all_of, cut = P(None, None, None), P(None, "dp", None)
    step = jax.shard_map(
        step,
        mesh=mesh,
        in_specs=(P(("rep", "dp"), None, None, None),) * 3 + (all_of,) * 3 + (cut,) * 6,
        out_specs=(P("rep", None, None),) * 3 + (P("rep", "dp", None),) * 6,
        check_vma=False,
    )
    return step
```

```python
import functools

import jax
import jax.numpy as jnp
from jax import lax
from jax.experimental import pallas as pl
from jax.experimental.pallas import tpu as pltpu
from jax.sharding import PartitionSpec as P


CORES = 2
SUBLANES = 8
SHORT = 2
VMEM_LIMIT = 20 * 2**20


def adamw(w, m, v, g):
    m = 0.9 * m + 0.1 * g
    v = 0.95 * v + 0.05 * g * g
    step = m * lax.rsqrt(v + 1e-8) + 0.1 * w
    return (w - 0.02 * step).astype(jnp.bfloat16), m, v


def cuts(rows):
    a = max(rows // 8, 1)
    b = max(rows // 3, a + 1)
    return (0, a), (a, b - a), (b, rows - b)


def kernel(n, order, late, *refs):
    units = len(order)
    g, w, m_in, v_in, out, m, v = (refs[i * units : (i + 1) * units] for i in range(7))
    after, refs = refs[7 * units : 7 * units + 2], refs[7 * units + 2 :]
    own, part, w_own = (refs[i * units : (i + 1) * units] for i in range(3))
    across_send, ring_send, ring_recv, pass_recv, short_sem = refs[3 * units :]

    me = lax.axis_index("dp")
    z, core = me // CORES, me % CORES
    ring = n // CORES
    partner = z * CORES + 1 - core
    last = ring - 1
    ways = (0, 1)
    lead, *others = order
    tail = order[-1]

    def chip(offset):
        return lax.rem(z + offset + 2 * ring, ring)

    def behind(d, j):
        return chip(j if d else -j)

    def owner(d, k):
        return behind(d, k + 1)

    def to(index):
        return {"device_id": {"dp": index}, "device_id_type": pl.DeviceIdType.MESH}

    def following(d):
        return to(behind(d, -1) * CORES + core)

    def wait_bytes(ref, sem):
        pltpu.make_async_copy(ref, ref, sem).wait()

    def push(d, k, u, sem, rows=slice(None)):
        pltpu.make_async_remote_copy(
            g[u].at[d, owner(d, k) * CORES + 1 - core, rows], part[u].at[d, k, rows], across_send.at[u], sem, **to(partner)
        ).start()

    def send(block, d, t, u, rows=slice(None), sem=None):
        piece = out[u].at[d, block, rows]
        sem = ring_recv.at[lax.rem(t, 3), d, u] if sem is None else sem
        pltpu.make_async_remote_copy(piece, piece, ring_send.at[u], sem, **following(d)).start()

    def sent(u):
        wait_bytes(out[u].at[:, 0], ring_send.at[u])

    def arrived(block, d, t, u):
        wait_bytes(out[u].at[d, block], ring_recv.at[lax.rem(t, 3), d, u])

    def pass_on(block, d, u, rows=slice(None)):
        piece = out[u].at[d, block, rows]
        pltpu.make_async_remote_copy(piece, piece, across_send.at[u], pass_recv.at[u], **to(partner)).start()

    def terms(slot, d, k, u, row):
        return own[u][slot, d, row].astype(jnp.float32) + part[u][d, k, row].astype(jnp.float32)

    rows_of = [x.shape[2] for x in own]

    def sums(own_sem, state_sem, push_recv, first_recv):
        def load_own(k, u):
            slot = lax.rem(k, 2)
            for d in ways:
                pltpu.make_async_copy(g[u].at[d, owner(d, k) * CORES + core], own[u].at[slot, d], own_sem.at[slot, u]).start()

        def push_all(k, u):
            for d in ways:
                push(d, k, u, push_recv.at[k, u])

        def terms_here(k, u):
            wait_bytes(own[u].at[lax.rem(k, 2)], own_sem.at[lax.rem(k, 2), u])
            wait_bytes(part[u].at[:, k], push_recv.at[k, u])

        for u in order:
            load_own(0, u)

        barrier = pltpu.get_barrier_semaphore()
        for index in (chip(1) * CORES + core, chip(-1) * CORES + core, partner):
            pl.semaphore_signal(barrier, inc=1, **to(index))
        pl.semaphore_wait(barrier, 3)

        for p, (at, count) in enumerate(cuts(rows_of[lead])):
            for d in ways:
                push(d, 0, lead, first_recv.at[d, p], pl.ds(at, count))
        for u in others:
            push_all(0, u)
        for u in order:
            load_own(1, u)
            push_all(1, u)

        def begin(d, u, at, count):
            block = owner(d, 0) * CORES + core

            @pl.loop(at, at + count)
            def _(row):
                out[u][d, block, row] = terms(0, d, 0, u, row).astype(out[u].dtype)

            send(block, d, 0, u, pl.ds(at, count))

        wait_bytes(own[lead].at[0], own_sem.at[0, lead])
        for p, (at, count) in enumerate(cuts(rows_of[lead])):
            for d in ways:
                wait_bytes(part[lead].at[d, 0, pl.ds(at, count)], first_recv.at[d, p])
                begin(d, lead, at, count)
        for u in others:
            terms_here(0, u)
            for d in ways:
                begin(d, u, 0, rows_of[u])

        state = {}
        for u in order:
            state[u] = (
                pltpu.make_async_copy(w[u].at[:, me], w_own[u], state_sem.at[0, u]),
                pltpu.make_async_copy(m_in[u], m[u], state_sem.at[1, u]),
                pltpu.make_async_copy(v_in[u], v[u], state_sem.at[2, u]),
            )
            for copy in state[u]:
                copy.start()

        @pl.loop(1, last)
        def _(k):
            slot = lax.rem(k, 2)
            for u in order:
                load_own(k + 1, u)
                push_all(k + 1, u)
            for u in order:
                terms_here(k, u)
                for d in ways:
                    block = owner(d, k) * CORES + core
                    arrived(block, d, k - 1, u)

                    @pl.loop(0, rows_of[u])
                    def _(row):
                        total = out[u][d, block, row].astype(jnp.float32) + terms(slot, d, k, u, row)
                        out[u][d, block, row] = total.astype(out[u].dtype)

                    if d == 0:
                        sent(u)
                    send(block, d, k, u)

        for u in order:
            terms_here(last, u)
            for copy in state[u]:
                copy.wait()
            for d in ways:
                arrived(me, d, last - 1, u)

                @pl.loop(0, rows_of[u])
                def _(row):
                    total = out[u][d, me, row].astype(jnp.float32) + terms(last % 2, d, last, u, row)
                    gradient = total.astype(jnp.bfloat16).astype(jnp.float32)
                    new = adamw(w_own[u][d, row].astype(jnp.float32), m[u][d, row], v[u][d, row], gradient)
                    out[u][d, me, row], m[u][d, row], v[u][d, row] = new

                if d == 0:
                    sent(u)
                send(me, d, last, u)
                pass_on(me, d, u)

    dma = lambda *shape: pltpu.SemaphoreType.DMA(shape)
    pl.run_scoped(sums, dma(2, units), dma(3, units), dma(ring, units), dma(2, len(cuts(rows_of[lead]))))

    rest = pl.ds(SHORT, rows_of[lead] - SHORT)

    def forward(d, j, u, rows=slice(None)):
        block = behind(d, j) * CORES + core
        arrived(block, d, last + j - 1, u)
        if d == 0:
            sent(u)
        send(block, d, last + j, u, rows)
        pass_on(block, d, u)

    for u in order:
        for d in ways:
            forward(d, 1, u)
        if u == lead:
            piece = out[u].at[0, me, pl.ds(0, SHORT)]
            short = pltpu.make_async_remote_copy(piece, piece, short_sem.at[0], short_sem.at[1], **following(1))
            short.start()

    @pl.loop(2, last - 2)
    def _(j):
        for u in order:
            for d in ways:
                forward(d, j, u)

    for u in order:
        if u == tail:
            for d in ways:
                forward(d, last - 1, lead, slice(None) if d else rest)
        for d in ways:
            forward(d, last - 2, u)

    for u in others:
        if u == tail:
            for d in ways:
                block = behind(d, last) * CORES + core
                if d == 0:
                    wait_bytes(out[lead].at[d, block, rest], ring_recv.at[(2 * last - 1) % 3, d, lead])
                    wait_bytes(out[lead].at[d, block, pl.ds(0, SHORT)], short_sem.at[1])
                else:
                    arrived(block, d, 2 * last - 1, lead)
                pass_on(block, d, lead)
        for d in ways:
            block = behind(d, last - 1) * CORES + core
            arrived(block, d, 2 * last - 2, u)

            @pl.loop(0, rows_of[u])
            def _(row):
                after[d][late.index(u), row] = out[u][d, block, row]

    short.wait_send()
    for u in order:
        if u == lead:
            wait_bytes(out[u].at[0, pl.ds(0, 2), pl.ds(0, rows_of[u] - SHORT // 2)], ring_send.at[u])
        else:
            sent(u)
        passed = last - 1 if u in late else ring
        wait_bytes(out[u].at[:, pl.ds(0, ring + passed)], across_send.at[u])
        wait_bytes(out[u].at[:, pl.ds(0, passed)], pass_recv.at[u])


def place(*refs):
    count = (len(refs) - 1) // 2
    copies = [pltpu.make_async_copy(refs[i], refs[count + i], refs[-1].at[i]) for i in range(count)]
    for copy in copies:
        copy.start()
    for copy in copies:
        copy.wait()


def put(n, late, where, *refs):
    count = len(late)
    blocks, out, sem = refs[count : count + len(where)], refs[-1 - count : -1], refs[-1]
    me = lax.axis_index("dp")
    z, core = me // CORES, me % CORES
    ring = n // CORES
    copies = []
    for part, (d, back, partners) in zip(blocks, where, strict=True):
        index = lax.rem(z + (back if d else ring - back), ring) * CORES + (1 - core if partners else core)
        copies += [pltpu.make_async_copy(part.at[i], out[i].at[d, index], sem.at[len(copies) + i]) for i in range(count)]
    for copy in copies:
        copy.start()
    for copy in copies:
        copy.wait()


def marker(ref, out):
    out[...] = jnp.zeros_like(out)


def solution(mesh):
    n = mesh.shape["dp"]

    def step(*arrays):
        return whole_step(*arrays)

    def whole_step(*arrays):
        terms, weights, m, v = (arrays[i : i + 3] for i in (0, 3, 6, 9))
        units = len(terms)
        order, late = (2, 0, 1), (0, 1)
        layers = weights[0].shape[0]

        def blocks(x, count):
            return x.reshape(layers, *([count] if count else []), -1, SUBLANES, x.shape[-1])

        terms = [blocks(t[0], n) for t in terms]
        weights_in = [blocks(x, n) for x in weights]
        m_in = [blocks(x, 0) for x in m]
        v_in = [blocks(x, 0) for x in v]
        ring = n // CORES
        block = [x.shape[1:] for x in m_in]
        dma = lambda *shape: pltpu.SemaphoreType.DMA(shape)
        new = pl.pallas_call(
            functools.partial(kernel, n, order, late),
            out_shape=[
                *(pltpu.VMEM(x.shape, x.dtype) for x in (*weights_in, *m_in, *v_in)),
                *[pltpu.VMEM((len(late), *block[late[0]]), jnp.bfloat16)] * 2,
            ],
            in_specs=[pl.BlockSpec(memory_space=pltpu.HBM)] * (4 * units),
            out_specs=[pl.BlockSpec(memory_space=pltpu.VMEM)] * (3 * units + 2),
            scratch_shapes=[
                *(pltpu.VMEM((2, 2, *b), jnp.bfloat16) for b in block),
                *(pltpu.VMEM((2, ring, *b), jnp.bfloat16) for b in block),
                *(pltpu.VMEM((2, *b), jnp.bfloat16) for b in block),
                dma(units),
                dma(units),
                dma(3, 2, units),
                dma(units),
                dma(2),
            ],
            compiler_params=pltpu.CompilerParams(collective_id=0, has_side_effects=True, vmem_limit_bytes=VMEM_LIMIT),
            name="step_end",
        )(*(pltpu.with_memory_space_constraint(x, pltpu.HBM) for x in (*terms, *weights_in, *m_in, *v_in)))
        new, after = new[: 3 * units], new[3 * units :]
        across = [(i, i ^ 1) for i in range(n)]
        far = []
        for d, way in enumerate((1, -1)):
            far.append(lax.ppermute(after[d], "dp", [(i, (i + way * CORES) % n) for i in range(n)]))
        near = [lax.ppermute(x, "dp", across) for x in after]
        writer = pl.pallas_call(
            place,
            out_shape=[jax.ShapeDtypeStruct(x.shape, x.dtype) for x in new],
            in_specs=[pl.BlockSpec(memory_space=pltpu.VMEM)] * len(new),
            out_specs=[pl.BlockSpec(memory_space=pltpu.HBM)] * len(new),
            scratch_shapes=[dma(len(new))],
            compiler_params=pltpu.CompilerParams(vmem_limit_bytes=VMEM_LIMIT),
            name="place",
            cost_estimate=pl.CostEstimate(flops=3 * 10**9, bytes_accessed=4 * 10**7, transcendentals=0),
        )
        new = list(writer(*(pltpu.with_memory_space_constraint(x, pltpu.VMEM) for x in new)))
        last = n // CORES - 1

        def write(parts, where):
            done = pl.pallas_call(
                functools.partial(put, n, late, where),
                out_shape=[jax.ShapeDtypeStruct(new[u].shape, new[u].dtype) for u in late],
                in_specs=[pl.BlockSpec(memory_space=pltpu.HBM)] * len(late) + [pl.BlockSpec(memory_space=pltpu.VMEM)] * len(parts),
                out_specs=[pl.BlockSpec(memory_space=pltpu.HBM)] * len(late),
                scratch_shapes=[dma(len(where) * len(late))],
                input_output_aliases={i: i for i in range(len(late))},
                compiler_params=pltpu.CompilerParams(vmem_limit_bytes=VMEM_LIMIT),
                cost_estimate=pl.CostEstimate(flops=2 * 10**8, bytes_accessed=2 * 10**6, transcendentals=0),
                name="put",
            )(*(new[u] for u in late), *(pltpu.with_memory_space_constraint(x, pltpu.VMEM) for x in parts))
            for u, x in zip(late, done, strict=True):
                new[u] = x

        def swap(d):
            far[d], new[late[0]] = lax.optimization_barrier((far[d], new[late[0]]))
            return lax.ppermute(far[d], "dp", across)

        swapped = {1: swap(1)}
        mark = pl.pallas_call(
            marker,
            out_shape=pltpu.VMEM((SUBLANES, 128), jnp.float32),
            in_specs=[pl.BlockSpec(memory_space=pltpu.VMEM)],
            out_specs=pl.BlockSpec(memory_space=pltpu.VMEM),
            compiler_params=pltpu.CompilerParams(vmem_limit_bytes=VMEM_LIMIT),
            cost_estimate=pl.CostEstimate(flops=10**5, bytes_accessed=10**4, transcendentals=0),
            name="mark",
        )(far[1])
        far[0], mark = lax.optimization_barrier((far[0], mark))
        swapped[0] = swap(0)
        write((*far, *near, mark), ((0, last, 0), (1, last, 0), (0, last - 1, 1), (1, last - 1, 1)))
        write((swapped[0], swapped[1]), ((0, last, 1), (1, last, 1)))
        return tuple(x.reshape(like.shape) for x, like in zip(new, (*weights, *m, *v), strict=True))

    all_of, cut = P(None, None, None), P(None, "dp", None)
    step = jax.shard_map(
        step,
        mesh=mesh,
        in_specs=(P(("rep", "dp"), None, None, None),) * 3 + (all_of,) * 3 + (cut,) * 6,
        out_specs=(P("rep", None, None),) * 3 + (P("rep", "dp", None),) * 6,
        check_vma=False,
    )
    return step
```

```python
import functools

import jax
import jax.numpy as jnp
from jax import lax
from jax.experimental import pallas as pl
from jax.experimental.pallas import tpu as pltpu
from jax.sharding import PartitionSpec as P


CORES = 2
SUBLANES = 8
SHORT = 2
VMEM_LIMIT = 20 * 2**20


def adamw(w, m, v, g):
    m = 0.9 * m + 0.1 * g
    v = 0.95 * v + 0.05 * g * g
    step = m * lax.rsqrt(v + 1e-8) + 0.1 * w
    return (w - 0.02 * step).astype(jnp.bfloat16), m, v


def cuts(rows):
    a = max(rows // 8, 1)
    b = max(rows // 3, a + 1)
    return (0, a), (a, b - a), (b, rows - b)


def kernel(n, order, late, *refs):
    units = len(order)
    g, w, m_in, v_in, out, m, v = (refs[i * units : (i + 1) * units] for i in range(7))
    after, refs = refs[7 * units : 7 * units + 2], refs[7 * units + 2 :]
    own, part, w_own = (refs[i * units : (i + 1) * units] for i in range(3))
    last_send, last_recv = refs[3 * units :]

    me = lax.axis_index("dp")
    z, core = me // CORES, me % CORES
    ring = n // CORES
    partner = z * CORES + 1 - core
    last = ring - 1
    ways = (0, 1)
    lead, *others = order
    tail = order[-1]
    rows_of = [x.shape[2] for x in own]

    def chip(offset):
        return lax.rem(z + offset + 2 * ring, ring)

    def behind(d, j):
        return chip(j if d else -j)

    def owner(d, k):
        return behind(d, k + 1)

    def to(index):
        return {"device_id": {"dp": index}, "device_id_type": pl.DeviceIdType.MESH}

    def following(d):
        return to(behind(d, -1) * CORES + core)

    def wait_bytes(ref, sem):
        pltpu.make_async_copy(ref, ref, sem).wait()

    def hand_over(d, u):
        block = behind(d, last - 1) * CORES + core

        @pl.loop(0, rows_of[u])
        def _(row):
            after[d][late.index(u), row] = out[u][d, block, row]

    dma = lambda *shape: pltpu.SemaphoreType.DMA(shape)

    def rings(across_send, ring_send, ring_recv, pass_recv, short_sem):
        def push(d, k, u, sem, rows=slice(None)):
            pltpu.make_async_remote_copy(
                g[u].at[d, owner(d, k) * CORES + 1 - core, rows], part[u].at[d, k, rows], across_send.at[u], sem, **to(partner)
            ).start()

        def send(block, d, t, u, rows=slice(None)):
            piece = out[u].at[d, block, rows]
            closing = u == tail and isinstance(t, int) and t == 2 * last - 2
            sems = (last_send, last_recv.at[d]) if closing else (ring_send.at[u], ring_recv.at[lax.rem(t, 3), d, u])
            pltpu.make_async_remote_copy(piece, piece, *sems, **following(d)).start()

        def sent(u):
            wait_bytes(out[u].at[:, 0], ring_send.at[u])

        def arrived(block, d, t, u):
            wait_bytes(out[u].at[d, block], ring_recv.at[lax.rem(t, 3), d, u])

        def pass_on(block, d, u, rows=slice(None)):
            piece = out[u].at[d, block, rows]
            pltpu.make_async_remote_copy(piece, piece, across_send.at[u], pass_recv.at[u], **to(partner)).start()

        def terms(slot, d, k, u, row):
            return own[u][slot, d, row].astype(jnp.float32) + part[u][d, k, row].astype(jnp.float32)

        def sums(own_sem, state_sem, push_recv, first_recv):
            def load_own(k, u):
                slot = lax.rem(k, 2)
                for d in ways:
                    pltpu.make_async_copy(g[u].at[d, owner(d, k) * CORES + core], own[u].at[slot, d], own_sem.at[slot, u]).start()

            def push_all(k, u):
                for d in ways:
                    push(d, k, u, push_recv.at[k, u])

            def terms_here(k, u):
                wait_bytes(own[u].at[lax.rem(k, 2)], own_sem.at[lax.rem(k, 2), u])
                wait_bytes(part[u].at[:, k], push_recv.at[k, u])

            for u in order:
                load_own(0, u)

            barrier = pltpu.get_barrier_semaphore()
            for index in (chip(1) * CORES + core, chip(-1) * CORES + core, partner):
                pl.semaphore_signal(barrier, inc=1, **to(index))
            pl.semaphore_wait(barrier, 3)

            for p, (at, count) in enumerate(cuts(rows_of[lead])):
                for d in ways:
                    push(d, 0, lead, first_recv.at[d, p], pl.ds(at, count))
            for u in others:
                push_all(0, u)
            for u in order:
                load_own(1, u)
                push_all(1, u)

            def begin(d, u, at, count):
                block = owner(d, 0) * CORES + core

                @pl.loop(at, at + count)
                def _(row):
                    out[u][d, block, row] = terms(0, d, 0, u, row).astype(out[u].dtype)

                send(block, d, 0, u, pl.ds(at, count))

            wait_bytes(own[lead].at[0], own_sem.at[0, lead])
            for p, (at, count) in enumerate(cuts(rows_of[lead])):
                for d in ways:
                    wait_bytes(part[lead].at[d, 0, pl.ds(at, count)], first_recv.at[d, p])
                    begin(d, lead, at, count)
            for u in others:
                terms_here(0, u)
                for d in ways:
                    begin(d, u, 0, rows_of[u])

            state = {}
            for u in order:
                state[u] = (
                    pltpu.make_async_copy(w[u].at[:, me], w_own[u], state_sem.at[0, u]),
                    pltpu.make_async_copy(m_in[u], m[u], state_sem.at[1, u]),
                    pltpu.make_async_copy(v_in[u], v[u], state_sem.at[2, u]),
                )
                for copy in state[u]:
                    copy.start()

            @pl.loop(1, last)
            def _(k):
                slot = lax.rem(k, 2)
                for u in order:
                    load_own(k + 1, u)
                    push_all(k + 1, u)
                for u in order:
                    terms_here(k, u)
                    for d in ways:
                        block = owner(d, k) * CORES + core
                        arrived(block, d, k - 1, u)

                        @pl.loop(0, rows_of[u])
                        def _(row):
                            total = out[u][d, block, row].astype(jnp.float32) + terms(slot, d, k, u, row)
                            out[u][d, block, row] = total.astype(out[u].dtype)

                        if d == 0:
                            sent(u)
                        send(block, d, k, u)

            for u in order:
                terms_here(last, u)
                for copy in state[u]:
                    copy.wait()
                for d in ways:
                    arrived(me, d, last - 1, u)

                    @pl.loop(0, rows_of[u])
                    def _(row):
                        total = out[u][d, me, row].astype(jnp.float32) + terms(last % 2, d, last, u, row)
                        gradient = total.astype(jnp.bfloat16).astype(jnp.float32)
                        new = adamw(w_own[u][d, row].astype(jnp.float32), m[u][d, row], v[u][d, row], gradient)
                        out[u][d, me, row], m[u][d, row], v[u][d, row] = new

                    if d == 0:
                        sent(u)
                    send(me, d, last, u)
                    pass_on(me, d, u)

        pl.run_scoped(sums, dma(2, units), dma(3, units), dma(ring, units), dma(2, len(cuts(rows_of[lead]))))

        rest = pl.ds(SHORT, rows_of[lead] - SHORT)

        def forward(d, j, u, rows=slice(None)):
            block = behind(d, j) * CORES + core
            arrived(block, d, last + j - 1, u)
            if d == 0:
                sent(u)
            send(block, d, last + j, u, rows)
            pass_on(block, d, u)

        for u in order:
            for d in ways:
                forward(d, 1, u)
            if u == lead:
                piece = out[u].at[0, me, pl.ds(0, SHORT)]
                short = pltpu.make_async_remote_copy(piece, piece, short_sem.at[0], short_sem.at[1], **following(1))
                short.start()

        @pl.loop(2, last - 2)
        def _(j):
            for u in order:
                for d in ways:
                    forward(d, j, u)

        for u in order:
            if u == tail:
                for d in ways:
                    forward(d, last - 1, lead, slice(None) if d else rest)
            for d in ways:
                forward(d, last - 2, u)

        for u in others[:-1]:
            for d in ways:
                arrived(behind(d, last - 1) * CORES + core, d, 2 * last - 2, u)
                hand_over(d, u)
        block = behind(0, last) * CORES + core
        wait_bytes(out[lead].at[0, block, rest], ring_recv.at[(2 * last - 1) % 3, 0, lead])
        wait_bytes(out[lead].at[0, block, pl.ds(0, SHORT)], short_sem.at[1])
        pass_on(block, 0, lead)
        block = behind(1, last) * CORES + core
        arrived(block, 1, 2 * last - 1, lead)
        pass_on(block, 1, lead)

        short.wait_send()
        for u in order:
            if u == lead:
                wait_bytes(out[u].at[0, pl.ds(0, 2), pl.ds(0, rows_of[u] - SHORT // 2)], ring_send.at[u])
            elif u != tail:
                sent(u)
            passed = last - 1 if u in late else ring
            wait_bytes(out[u].at[:, pl.ds(0, ring + passed)], across_send.at[u])
            wait_bytes(out[u].at[:, pl.ds(0, passed)], pass_recv.at[u])

    pl.run_scoped(rings, dma(units), dma(units), dma(3, 2, units), dma(units), dma(2))

    for d in ways[::-1]:
        wait_bytes(out[tail].at[d, behind(d, last - 1) * CORES + core], last_recv.at[d])
        hand_over(d, tail)
    wait_bytes(out[tail].at[:, 0], last_send)


def place(*refs):
    count = (len(refs) - 1) // 2
    copies = [pltpu.make_async_copy(refs[i], refs[count + i], refs[-1].at[i]) for i in range(count)]
    for copy in copies:
        copy.start()
    for copy in copies:
        copy.wait()


def put(n, late, where, *refs):
    count = len(late)
    blocks, out, sem = refs[count : count + len(where)], refs[-1 - count : -1], refs[-1]
    me = lax.axis_index("dp")
    z, core = me // CORES, me % CORES
    ring = n // CORES
    copies = []
    for part, (d, back, partners) in zip(blocks, where, strict=True):
        index = lax.rem(z + (back if d else ring - back), ring) * CORES + (1 - core if partners else core)
        copies += [pltpu.make_async_copy(part.at[i], out[i].at[d, index], sem.at[len(copies) + i]) for i in range(count)]
    for copy in copies:
        copy.start()
    for copy in copies:
        copy.wait()


def marker(ref, out):
    out[...] = jnp.zeros_like(out)


def solution(mesh):
    n = mesh.shape["dp"]

    def step(*arrays):
        return whole_step(*arrays)

    def whole_step(*arrays):
        terms, weights, m, v = (arrays[i : i + 3] for i in (0, 3, 6, 9))
        units = len(terms)
        order, late = (2, 0, 1), (0, 1)
        layers = weights[0].shape[0]

        def blocks(x, count):
            return x.reshape(layers, *([count] if count else []), -1, SUBLANES, x.shape[-1])

        terms = [blocks(t[0], n) for t in terms]
        weights_in = [blocks(x, n) for x in weights]
        m_in = [blocks(x, 0) for x in m]
        v_in = [blocks(x, 0) for x in v]
        ring = n // CORES
        block = [x.shape[1:] for x in m_in]
        dma = lambda *shape: pltpu.SemaphoreType.DMA(shape)
        new = pl.pallas_call(
            functools.partial(kernel, n, order, late),
            out_shape=[
                *(pltpu.VMEM(x.shape, x.dtype) for x in (*weights_in, *m_in, *v_in)),
                *[pltpu.VMEM((len(late), *block[late[0]]), jnp.bfloat16)] * 2,
            ],
            in_specs=[pl.BlockSpec(memory_space=pltpu.HBM)] * (4 * units),
            out_specs=[pl.BlockSpec(memory_space=pltpu.VMEM)] * (3 * units + 2),
            scratch_shapes=[
                *(pltpu.VMEM((2, 2, *b), jnp.bfloat16) for b in block),
                *(pltpu.VMEM((2, ring, *b), jnp.bfloat16) for b in block),
                *(pltpu.VMEM((2, *b), jnp.bfloat16) for b in block),
                pltpu.SemaphoreType.DMA,
                dma(2),
            ],
            compiler_params=pltpu.CompilerParams(collective_id=0, has_side_effects=True, vmem_limit_bytes=VMEM_LIMIT),
            name="step_end",
        )(*(pltpu.with_memory_space_constraint(x, pltpu.HBM) for x in (*terms, *weights_in, *m_in, *v_in)))
        new, after = new[: 3 * units], new[3 * units :]
        across = [(i, i ^ 1) for i in range(n)]
        far = []
        for d, way in enumerate((1, -1)):
            far.append(lax.ppermute(after[d], "dp", [(i, (i + way * CORES) % n) for i in range(n)]))
        near = [lax.ppermute(x, "dp", across) for x in after]
        writer = pl.pallas_call(
            place,
            out_shape=[jax.ShapeDtypeStruct(x.shape, x.dtype) for x in new],
            in_specs=[pl.BlockSpec(memory_space=pltpu.VMEM)] * len(new),
            out_specs=[pl.BlockSpec(memory_space=pltpu.HBM)] * len(new),
            scratch_shapes=[dma(len(new))],
            compiler_params=pltpu.CompilerParams(vmem_limit_bytes=VMEM_LIMIT),
            name="place",
            cost_estimate=pl.CostEstimate(flops=3 * 10**9, bytes_accessed=4 * 10**7, transcendentals=0),
        )
        new = list(writer(*(pltpu.with_memory_space_constraint(x, pltpu.VMEM) for x in new)))
        last = n // CORES - 1

        def write(parts, where):
            done = pl.pallas_call(
                functools.partial(put, n, late, where),
                out_shape=[jax.ShapeDtypeStruct(new[u].shape, new[u].dtype) for u in late],
                in_specs=[pl.BlockSpec(memory_space=pltpu.HBM)] * len(late) + [pl.BlockSpec(memory_space=pltpu.VMEM)] * len(parts),
                out_specs=[pl.BlockSpec(memory_space=pltpu.HBM)] * len(late),
                scratch_shapes=[dma(len(where) * len(late))],
                input_output_aliases={i: i for i in range(len(late))},
                compiler_params=pltpu.CompilerParams(vmem_limit_bytes=VMEM_LIMIT),
                cost_estimate=pl.CostEstimate(flops=2 * 10**8, bytes_accessed=2 * 10**6, transcendentals=0),
                name="put",
            )(*(new[u] for u in late), *(pltpu.with_memory_space_constraint(x, pltpu.VMEM) for x in parts))
            for u, x in zip(late, done, strict=True):
                new[u] = x

        def swap(d):
            far[d], new[late[0]] = lax.optimization_barrier((far[d], new[late[0]]))
            return lax.ppermute(far[d], "dp", across)

        swapped = {1: swap(1)}
        mark = pl.pallas_call(
            marker,
            out_shape=pltpu.VMEM((SUBLANES, 128), jnp.float32),
            in_specs=[pl.BlockSpec(memory_space=pltpu.VMEM)],
            out_specs=pl.BlockSpec(memory_space=pltpu.VMEM),
            compiler_params=pltpu.CompilerParams(vmem_limit_bytes=VMEM_LIMIT),
            cost_estimate=pl.CostEstimate(flops=10**5, bytes_accessed=10**4, transcendentals=0),
            name="mark",
        )(far[1])
        far[0], mark = lax.optimization_barrier((far[0], mark))
        swapped[0] = swap(0)
        write((*far, *near, mark), ((0, last, 0), (1, last, 0), (0, last - 1, 1), (1, last - 1, 1)))
        write((swapped[0], swapped[1]), ((0, last, 1), (1, last, 1)))
        return tuple(x.reshape(like.shape) for x, like in zip(new, (*weights, *m, *v), strict=True))

    all_of, cut = P(None, None, None), P(None, "dp", None)
    step = jax.shard_map(
        step,
        mesh=mesh,
        in_specs=(P(("rep", "dp"), None, None, None),) * 3 + (all_of,) * 3 + (cut,) * 6,
        out_specs=(P("rep", None, None),) * 3 + (P("rep", "dp", None),) * 6,
        check_vma=False,
    )
    return step
```
